256 devices in a mesh: member: 4 (over y, x), gx: 64 (over z, core).
Axes of the slice: x: 2, y: 2, z: 32, core: 2. Of those that a mesh axis runs over, the one named last changes fastest.
The devices are a block of a 4x8x32 slice.
Arguments:
- spectrum: float32 [36, 32, 2048, 128], P(None, None, ('member', 'gx')), parts along dimension 2, may hold values from 0 to 1
- wind: float32 [2, 2048, 128], P(None, ('member', 'gx')), parts along dimension 1, may hold values from -32 to 32
- land_sea: int32 [512, 128], P('gx'), may hold values 0 or 1
- band_rows: int32 [128], replicated, may hold values from 0 to 127, each once
Outputs:
- spectrum_next: float32 [36, 32, 2048, 128], P(None, None, ('member', 'gx')), parts along dimension 2
- ocean_fields: float32 [4, 128, 2048], P(None, 'gx', 'member'), parts along dimension 2
The draws below stay inside these ranges and needn't reach their ends.
There are 4 independent parts, one for each index of `member`. The reference program is written for one: setup_inputs(seed, part) draws one part's arguments, and reference() takes and returns one part's arrays. A program takes and returns all parts, laid end to end along the dimension named above; an argument that names none is the same for every part. Nothing has to cross between parts.
Inputs may be any that keep to these rules, and one draw needn't show every extreme that they name: band_rows names each of the 128 latitude rows exactly once.
All inputs are finite; a program needn't handle non-finite values. No bound on the sum of `land_sea` on one device may be relied on, other than what follows from the above.
Results may differ from the reference program's by a relative error of at most 0.00015.
Values sent between devices are 32-bit elements; how exact they have to be, the bound alone decides.
A program may use at most 128 MiB of HBM per device.

```python
import math
import jax
import jax.numpy as jnp
from jax import lax

DIRS = 36
FREQS = 32
LAT = 128
STEPS = 3
NLON = 512


def touch_ends(values, key, least, largest):
    index_at = [jax.random.randint(jax.random.fold_in(key, axis), (), 0, length) for axis, length in enumerate(values.shape)]
    longest = values.shape.index(max(values.shape))
    beside = index_at[:longest] + [(index_at[longest] + 1) % values.shape[longest]] + index_at[longest + 1:]
    return values.at[tuple(index_at)].set(least).at[tuple(beside)].set(largest)


def block_levels(own_key, shape, shards, least, largest):
    def one(position, shards_of):
        draws = jax.random.uniform(jax.random.fold_in(jax.random.fold_in(own_key, 6), position), (shards_of,), jnp.float32, least / len(shards), largest / len(shards))
        return jnp.repeat(jnp.exp(draws), shape[position] // shards_of).reshape((-1,) + (1,) * (len(shape) - position - 1))

    loudness = one(*shards[0])
    for cut in shards[1:]:
        loudness = loudness * one(*cut)
    return loudness


def centred(rng, dims, width, bound, cuts=(), kind=jnp.bfloat16):
    level = block_levels(rng, dims, cuts, -0.22, 0.18) if cuts else 1.0
    array = jax.random.normal(rng, dims, jnp.float32) * width * level
    return jnp.minimum(jnp.maximum(array, -bound), bound).astype(kind)


def setup_inputs(seed: int = 0, part: int = 0) -> dict:
    keys = jax.random.split(jax.random.key(seed), 5)
    part_keys = jax.random.split(jax.random.fold_in(keys[4], part), 5)
    spectrum = jnp.clip(1.0 * jax.random.uniform(part_keys[0], (DIRS, FREQS, NLON, LAT), jnp.float32) ** block_levels(part_keys[0], (DIRS, FREQS, NLON, LAT), ((2, 64),), -0.2, 0.2), 0.0, 1.0)
    wind = centred(part_keys[1], (2, NLON, LAT), 8.0, 32.0, ((1, 64),), jnp.float32)
    land_sea = touch_ends((jax.random.randint(keys[2], (NLON, LAT), 0, 4) < 3).astype(jnp.int32), jax.random.fold_in(keys[2], 1), 0, 1)
    band_rows = jax.random.permutation(keys[3], LAT).astype(jnp.int32)
    return dict(spectrum=spectrum, wind=wind, land_sea=land_sea, band_rows=band_rows)


def wave_tables(directions, frequencies):
    angles = (jnp.arange(directions, dtype=jnp.float32) + 0.5) * (2.0 * math.pi / directions)
    levels = jnp.arange(frequencies, dtype=jnp.float32)
    shrink = jnp.power(jnp.float32(1.1), -levels)
    frequency = 0.0418 / shrink
    inverse_speed = 2.0 * math.pi * frequency / 9.81
    weight = (levels + 1.0) / frequencies
    cosine_dir = jnp.cos(angles)[:, None]
    sine_dir = jnp.sin(angles)[:, None]
    courant_x = 0.45 * shrink[None, :] * cosine_dir
    courant_y = 0.45 * shrink[None, :] * sine_dir
    factor = 3.0 / math.sqrt(directions * frequencies)
    project = jnp.stack([factor * weight[None, :] * cosine_dir, factor * weight[None, :] * sine_dir])
    return (courant_x, courant_y, cosine_dir, sine_dir, inverse_speed, weight * weight, project)

def upwind(center, west_cell, east_cell, courant_x, courant_y):
    along_x = courant_x[:, :, None, None]
    along_y = courant_y[:, :, None, None]
    border = jnp.zeros_like(center[..., :1])
    south_cell = jnp.concatenate([border, center[..., :-1]], axis=3)
    north_cell = jnp.concatenate([center[..., 1:], border], axis=3)
    return center - jnp.maximum(along_x, 0.0) * (center - west_cell) + jnp.maximum(-along_x, 0.0) * (east_cell - center) - jnp.maximum(along_y, 0.0) * (center - south_cell) + jnp.maximum(-along_y, 0.0) * (north_cell - center)

def sources(advected, wind_east, wind_north, sea_mask, tables):
    cosine_dir, sine_dir, inverse_speed, weight_two = (tables[2], tables[3], tables[4], tables[5])
    advected = advected * sea_mask
    energy = lax.optimization_barrier(jnp.mean(advected, axis=(0, 1)))
    wind_ratio = (wind_east * cosine_dir[:, :, None, None] + wind_north * sine_dir[:, :, None, None]) * inverse_speed[None, :, None, None]
    growth = 0.05 * jnp.clip(wind_ratio - 1.0, 0.0, 4.0)
    damping = 0.3 * weight_two[None, :, None, None] * (energy / (0.5 + energy))
    return (advected * (1.0 + growth) / (1.0 + damping), growth * advected)

def coupling_fields(input_flux, current, project):
    stress = jnp.einsum('cij,ijxy->cxy', project, input_flux, precision=lax.Precision.HIGHEST)
    stokes = jnp.einsum('cij,ijxy->cxy', project, current, precision=lax.Precision.HIGHEST)
    return jnp.concatenate([stress, stokes], axis=0)

def reference(spectrum, wind, land_sea, band_rows):
    tables = wave_tables(spectrum.shape[0], spectrum.shape[1])
    sea_mask = land_sea.astype(jnp.float32)
    current = spectrum
    for step_index in range(STEPS):
        advected = upwind(current, jnp.roll(current, 1, axis=2), jnp.roll(current, -1, axis=2), tables[0], tables[1])
        current, input_flux = sources(advected, wind[0], wind[1], sea_mask, tables)
    fields = coupling_fields(input_flux, current, tables[6])
    ocean_fields = jnp.transpose(fields[:, :, band_rows], (0, 2, 1))
    return (current, ocean_fields)
```

```python
import functools
import math

import jax
import jax.numpy as jnp
from jax import lax
from jax.experimental import pallas as pl
from jax.experimental.pallas import tpu as pltpu
from jax.sharding import PartitionSpec as P

STEPS = 3
EARLY = 5
MEMBER_GX = ("member", "gx")
MESH = pl.DeviceIdType.MESH


def freq_constants(freqs):
    out = []
    for j in range(freqs):
        shrink = 1.1 ** (-j)
        weight = (j + 1) / freqs
        inverse_speed = 2.0 * math.pi * (0.0418 / shrink) / 9.81
        out.append((0.45 * shrink, 0.05 * inverse_speed, weight, 0.3 * weight * weight))
    return out


def window_kernel(
    sizes,
    spectrum,
    wind,
    land,
    band,
    spectrum_out,
    ocean_out,
    buf,
    grow,
    grow_one,
    wind_v,
    land_v,
    band_v,
    trig,
    send_e,
    send_w,
    recv_e,
    recv_w,
    halo,
    damp,
    damp_edge,
    edge_send,
    edge_recv,
    stokes_c,
    stokes_s,
    place,
    turned,
    fields,
    message,
    arrived,
    load_sem,
    small_sem,
    store_sem,
    halo_send_sem,
    halo_recv_sem,
    edge_send_sem,
    edge_recv_sem,
    message_send_sem,
    message_recv_sem,
    known_sem,
):
    devices, quarter, freqs, lons, lats = sizes
    consts = freq_constants(freqs)
    me = lax.axis_index("gx")
    east = lax.rem(me + 1, devices)
    west = lax.rem(me + devices - 1, devices)

    def load(k):
        return pltpu.make_async_copy(spectrum.at[:, k], buf.at[:, k], load_sem.at[k])

    for k in range(quarter):
        load(k).start()
    small = [
        pltpu.make_async_copy(wind, wind_v, small_sem.at[0]),
        pltpu.make_async_copy(land, land_v, small_sem.at[1]),
        pltpu.make_async_copy(band, band_v, small_sem.at[2]),
    ]
    for copy in small:
        copy.start()

    barrier = pltpu.get_barrier_semaphore()
    for neighbour in (west, east):
        pl.semaphore_signal(barrier, inc=1, device_id={"gx": neighbour}, device_id_type=MESH)

    for k in range(quarter):
        angle = (k + 0.5) * 2.0 * math.pi / (4 * quarter)
        trig[k] = jnp.float32(math.cos(angle))
        trig[quarter + k] = jnp.float32(math.sin(angle))
    rows = lax.broadcasted_iota(jnp.int32, (lons, lats), 0)
    lanes = lax.broadcasted_iota(jnp.int32, (lons, lats), 1)
    first_row = rows == 0
    last_row = rows == lons - 1
    inner_south = jnp.where(lanes == 0, 0.0, 1.0)
    inner_north = jnp.where(lanes == lats - 1, 0.0, 1.0)
    stokes_c[...] = jnp.zeros_like(stokes_c)
    stokes_s[...] = jnp.zeros_like(stokes_s)
    turned[...] = jnp.zeros_like(turned)

    for copy in small:
        copy.wait()
    mask = land_v[...].astype(jnp.float32)
    wind_east = wind_v[0]
    wind_north = wind_v[1]

    pl.semaphore_wait(barrier, 2)

    def tell(n):
        reach = 2**n
        for other in (lax.rem(me + reach, devices), lax.rem(me + devices - reach, devices)):
            pl.semaphore_signal(known_sem.at[n], inc=1, device_id={"gx": other}, device_id_type=MESH)

    def hear(n):
        pl.semaphore_wait(known_sem.at[n], 2)

    rounds = int(math.log2(devices)) - 1
    tell(0)

    def halo_copy(s, k, to_east):
        src, dst, side, where = (send_e, recv_e, 0, east) if to_east else (send_w, recv_w, 1, west)
        return pltpu.make_async_remote_copy(
            src_ref=src.at[s, k],
            dst_ref=dst.at[s, k],
            send_sem=halo_send_sem.at[s, side, k],
            recv_sem=halo_recv_sem.at[s, side, k],
            device_id={"gx": where},
            device_id_type=MESH,
        )

    def edge_copy(s, to_east):
        side, where = (0, east) if to_east else (1, west)
        return pltpu.make_async_remote_copy(
            src_ref=edge_send.at[s, side],
            dst_ref=edge_recv.at[s, side],
            send_sem=edge_send_sem.at[s, side],
            recv_sem=edge_recv_sem.at[s, side],
            device_id={"gx": where},
            device_id_type=MESH,
        )

    def pack(s, k):
        last = pl.ds(lons - 1, freqs, stride=lons)
        first = pl.ds(0, freqs, stride=lons)
        send_e[s, k, :freqs] = buf[0, k, last]
        send_e[s, k, freqs:] = buf[3, k, last]
        send_w[s, k, :freqs] = buf[1, k, first]
        send_w[s, k, freqs:] = buf[2, k, first]

    def ship(s, k):
        halo_copy(s, k, True).start()
        halo_copy(s, k, False).start()

    @pl.loop(0, quarter)
    def _(k):
        load(k).wait()
        pack(0, k)
        ship(0, k)

    hear(0)
    if rounds > 1:
        tell(1)

    def one_step(s):
        def body(k, carry):
            energy, across, along = carry
            c = jnp.full((lons, lats), trig[k], jnp.float32)
            n = jnp.full((lons, lats), trig[quarter + k], jnp.float32)
            both = c + n
            c_south, n_south = c * inner_south, n * inner_south
            c_north, n_north = c * inner_north, n * inner_north
            halo_copy(s, k, True).wait_recv()
            halo_copy(s, k, False).wait_recv()
            if s > 0:
                from_west = damp_edge[0]
                from_east = damp_edge[1]
                halo[0, :freqs] = recv_e[s, k, :freqs] * from_west
                halo[0, freqs:] = recv_e[s, k, freqs:] * from_west
                halo[1, :freqs] = recv_w[s, k, :freqs] * from_east
                halo[1, freqs:] = recv_w[s, k, freqs:] * from_east
            else:
                blow = wind_east * c + wind_north * n
                cross = wind_north * c - wind_east * n
            sum_across = jnp.zeros((lons, lats), jnp.float32)
            sum_along = jnp.zeros((lons, lats), jnp.float32)
            energy = list(energy)
            for j in range(freqs):
                shrink, speed, weight, _ = consts[j]
                tile = pl.ds(j * lons, lons)
                if s > 0:
                    d = damp[tile]
                if s == 0:
                    ahead = blow * speed
                    aside = cross * speed
                    gains = (ahead - 0.05, aside - 0.05, -0.05 - ahead, -0.05 - aside)
                new, flux = [], []
                for q in range(4):
                    center = buf[q, k, tile]
                    if s > 0:
                        center = center * d
                    eastward = q in (0, 3)
                    southern = q < 2
                    row = j + (freqs if q in (2, 3) else 0)
                    if s > 0:
                        edge = halo[0 if eastward else 1, pl.ds(row, 1)]
                    else:
                        edge = (recv_e if eastward else recv_w)[s, k, pl.ds(row, 1)]
                    if eastward:
                        upwind_x = jnp.where(first_row, edge, pltpu.roll(center, 1, 0))
                    else:
                        upwind_x = jnp.where(last_row, edge, pltpu.roll(center, lons - 1, 0))
                    upwind_y = pltpu.roll(center, 1 if southern else lats - 1, 1)
                    c_in, n_in = (c_south, n_south) if southern else (c_north, n_north)
                    x_rate, y_rate = (c, n_in) if q in (0, 2) else (n, c_in)
                    moved = center - shrink * (both * center - x_rate * upwind_x - y_rate * upwind_y)
                    energy[q] = energy[q] + moved
                    if s == 0:
                        gain = mask * jnp.minimum(jnp.maximum(gains[q], 0.0), 0.2)
                        grow[q, k, tile] = gain
                        gain_one = gain + mask
                        grow_one[q, k, tile] = gain_one
                    else:
                        gain_one = grow_one[q, k, tile]
                    value = moved * gain_one
                    buf[q, k, tile] = value
                    if s == STEPS - 1:
                        new.append(value)
                        flux.append(moved * grow[q, k, tile])
                if s == STEPS - 1:
                    sum_across = sum_across + weight * (flux[0] - flux[2])
                    sum_along = sum_along + weight * (flux[1] - flux[3])
                    d02 = new[0] - new[2]
                    d13 = new[1] - new[3]
                    stokes_c[tile] = stokes_c[tile] + (c * d02 - n * d13)
                    stokes_s[tile] = stokes_s[tile] + (n * d02 + c * d13)
            across = across + (c * sum_across - n * sum_along)
            along = along + (n * sum_across + c * sum_along)
            if s < STEPS - 1:
                pack(s + 1, k)

                @pl.when(k < EARLY)
                def _():
                    ship(s + 1, k)

            return tuple(energy), across, along

        zero = jnp.zeros((lons, lats), jnp.float32)
        energy, across, along = lax.fori_loop(0, quarter, body, ((zero,) * 4, zero, zero))
        total = (energy[0] + energy[1]) + (energy[2] + energy[3])
        return mask * total * (1.0 / (4 * quarter * freqs)), across, along

    def set_damping(energy):
        ratio = energy / (0.5 + energy)
        for j in range(freqs):
            damp[pl.ds(j * lons, lons)] = 1.0 / (1.0 + consts[j][3] * ratio)

    edge_weight = (lax.broadcasted_iota(jnp.int32, (freqs, lats), 0).astype(jnp.float32) + 1.0) / freqs
    edge_weight = 0.3 * edge_weight * edge_weight

    for s in range(STEPS):
        energy, across, along = one_step(s)
        if s < STEPS - 1:
            edge_send[s, 0] = energy[lons - 1 :]
            edge_send[s, 1] = energy[:1]
            edge_copy(s, True).start()
            edge_copy(s, False).start()
            for k in range(EARLY, quarter):
                ship(s + 1, k)
        set_damping(energy)
        if s == 0:
            for n in range(1, min(3, rounds)):
                hear(n)
                if n + 1 < rounds:
                    tell(n + 1)
            lat = lax.broadcasted_iota(jnp.int32, (lats, lats), 0)
            place[...] = jnp.where(band_v[...] == lat, 1.0, 0.0).T
        if s == 1 and rounds > 3:
            hear(3)
            if rounds > 4:
                tell(4)
        if s < STEPS - 1:
            for side, to_east in ((0, True), (1, False)):
                edge_copy(s, to_east).wait_recv()
                other = edge_recv[s, side]
                ratio = other / (0.5 + other)
                damp_edge[side] = 1.0 / (1.0 + edge_weight * ratio)

    factor = 3.0 / math.sqrt(4 * quarter * freqs)
    drift_c = jnp.zeros((lons, lats), jnp.float32)
    drift_s = jnp.zeros((lons, lats), jnp.float32)
    for j in range(freqs):
        tile = pl.ds(j * lons, lons)
        d = damp[tile] * consts[j][2]
        drift_c = drift_c + d * stokes_c[tile]
        drift_s = drift_s + d * stokes_s[tile]
    parts = 4 * lons
    for c, value in enumerate((across, along, drift_c, drift_s)):
        value = factor * value
        turned[pl.ds(c * lons, lons), :lats] = value
        turned[pl.ds(parts + c * lons, lons), lats:] = value
    pick = jnp.concatenate(
        [place[pl.ds(0, devices, stride=2)], place[pl.ds(1, devices, stride=2)]], axis=1
    )
    message[:, 0, :] = lax.dot_general(
        pick,
        turned[...],
        (((1,), (1,)), ((), ())),
        precision=lax.Precision.HIGHEST,
        preferred_element_type=jnp.float32,
    )

    if rounds > 4:
        hear(4)

    def message_copy(offset):
        to = lax.rem(me + offset, devices)
        return pltpu.make_async_remote_copy(
            src_ref=message.at[to],
            dst_ref=arrived.at[me],
            send_sem=message_send_sem,
            recv_sem=message_recv_sem,
            device_id={"gx": to},
            device_id_type=MESH,
        )

    half = devices // 2
    message_copy(half).start()

    @pl.loop(1, half)
    def _(near):
        message_copy(half - near).start()
        message_copy(half + near).start()

    arrived[me] = message[me]

    def store(k):
        return pltpu.make_async_copy(buf.at[:, k], spectrum_out.at[:, k], store_sem.at[k])

    @pl.loop(0, quarter)
    def _(k):
        for j in range(freqs):
            tile = pl.ds(j * lons, lons)
            d = damp[tile]
            for q in range(4):
                buf[q, k, tile] = buf[q, k, tile] * d
        store(k).start()

    for s in range(STEPS):
        for k in range(quarter):
            halo_copy(s, k, True).wait_send()
            halo_copy(s, k, False).wait_send()
    for s in range(STEPS - 1):
        edge_copy(s, True).wait_send()
        edge_copy(s, False).wait_send()
    all_out = pltpu.make_async_remote_copy(
        src_ref=message.at[pl.ds(0, devices - 1)],
        dst_ref=arrived.at[pl.ds(0, devices - 1)],
        send_sem=message_send_sem,
        recv_sem=message_recv_sem,
        device_id={"gx": east},
        device_id_type=MESH,
    )
    all_out.wait_send()
    for k in range(quarter):
        store(k).wait()
    all_out.wait_recv()

    per = lats // lons
    block = lanes // lons
    for b in range(devices // per):
        pieces = []
        for h in range(per // 8):
            piece = arrived[pl.ds(b * per + h * 8, 8), 0, :]
            pieces.append(pltpu.roll(piece, h * 8 * lons, 1, stride=lons, stride_axis=0))
        for slot in range(8):
            total = jnp.zeros((8, lats), jnp.float32)
            for h, piece in enumerate(pieces):
                total = total + jnp.where(block == (slot + h * 8 + rows) % per, piece, 0.0)
            line = jnp.sum(total, axis=0, keepdims=True)
            if slot:
                line = pltpu.roll(jnp.broadcast_to(line, (8, lats)), lats - slot * lons, 1)[:1]
            r, c = divmod(slot, 4)
            ocean_out[pl.ds(c * 2 + r, 1), pl.ds(b * lats, lats)] = line


def solution(mesh):
    devices = mesh.shape["gx"]

    def per_device(spectrum, wind, land_sea, band_rows):
        dirs, freqs, lons, lats = spectrum.shape
        quarter = dirs // 4
        tiles = freqs * lons
        f32 = jnp.float32
        any_space = pl.BlockSpec(memory_space=pl.ANY)
        dma = pltpu.SemaphoreType.DMA
        next_spectrum, ocean = pl.pallas_call(
            functools.partial(window_kernel, (devices, quarter, freqs, lons, lats)),
            out_shape=(
                jax.ShapeDtypeStruct((4, quarter, tiles, lats), f32),
                jax.ShapeDtypeStruct((8, devices * lons), f32),
            ),
            in_specs=[any_space] * 4,
            out_specs=(any_space, pl.BlockSpec(memory_space=pltpu.VMEM)),
            scratch_shapes=[
                pltpu.VMEM((4, quarter, tiles, lats), f32),
                pltpu.VMEM((4, quarter, tiles, lats), f32),
                pltpu.VMEM((4, quarter, tiles, lats), f32),
                pltpu.VMEM((2, lons, lats), f32),
                pltpu.VMEM((lons, lats), jnp.int32),
                pltpu.VMEM((1, lats), jnp.int32),
                pltpu.SMEM((2 * quarter,), f32),
                pltpu.VMEM((STEPS, quarter, 2 * freqs, lats), f32),
                pltpu.VMEM((STEPS, quarter, 2 * freqs, lats), f32),
                pltpu.VMEM((STEPS, quarter, 2 * freqs, lats), f32),
                pltpu.VMEM((STEPS, quarter, 2 * freqs, lats), f32),
                pltpu.VMEM((2, 2 * freqs, lats), f32),
                pltpu.VMEM((tiles, lats), f32),
                pltpu.VMEM((2, freqs, lats), f32),
                pltpu.VMEM((STEPS - 1, 2, 1, lats), f32),
                pltpu.VMEM((STEPS - 1, 2, 1, lats), f32),
                pltpu.VMEM((tiles, lats), f32),
                pltpu.VMEM((tiles, lats), f32),
                pltpu.VMEM((lats, lats), f32),
                pltpu.VMEM((lats, 2 * lats), f32),
                pltpu.VMEM((8, lats), f32),
                pltpu.VMEM((devices, 1, lats), f32),
                pltpu.VMEM((devices, 1, lats), f32),
                dma((quarter,)),
                dma((3,)),
                dma((quarter,)),
                dma((STEPS, 2, quarter)),
                dma((STEPS, 2, quarter)),
                dma((STEPS - 1, 2)),
                dma((STEPS - 1, 2)),
                dma,
                dma,
                pltpu.SemaphoreType.REGULAR((5,)),
            ],
            compiler_params=pltpu.CompilerParams(collective_id=0, has_side_effects=True),
        )(
            spectrum.reshape(4, quarter, tiles, lats),
            wind,
            land_sea,
            band_rows.reshape(1, lats),
        )
        ocean = ocean.reshape(4, 2, devices * lons)
        return next_spectrum.reshape(spectrum.shape), ocean

    return jax.shard_map(
        per_device,
        mesh=mesh,
        in_specs=(P(None, None, MEMBER_GX, None), P(None, MEMBER_GX, None), P("gx", None), P(None)),
        out_specs=(P(None, None, MEMBER_GX, None), P(None, "gx", "member")),
        check_vma=False,
    )
```

```python
import functools
import math

import jax
import jax.numpy as jnp
from jax import lax
from jax.experimental import pallas as pl
from jax.experimental.pallas import tpu as pltpu
from jax.sharding import PartitionSpec as P

STEPS = 3
EARLY = 5
KERNEL_VMEM = 36 * 2**20
HEARD = ((0, 0), (0, 1), (0, 5), (1, 1))
MEMBER_GX = ("member", "gx")
MESH = pl.DeviceIdType.MESH


def freq_constants(freqs):
    out = []
    for j in range(freqs):
        shrink = 1.1 ** (-j)
        weight = (j + 1) / freqs
        inverse_speed = 2.0 * math.pi * (0.0418 / shrink) / 9.81
        out.append((0.45 * shrink, 0.05 * inverse_speed, weight, 0.3 * weight * weight))
    return out


def window_kernel(
    sizes,
    spectrum,
    wind,
    land,
    band,
    buf,
    arrived,
    grow,
    grow_one,
    wind_v,
    land_v,
    band_v,
    trig,
    send_e,
    send_w,
    recv_e,
    recv_w,
    halo,
    damp,
    damp_edge,
    edge_send,
    edge_recv,
    stokes_c,
    stokes_s,
    place,
    turned,
    message,
    load_sem,
    small_sem,
    halo_send_sem,
    halo_recv_sem,
    edge_send_sem,
    edge_recv_sem,
    message_send_sem,
    message_recv_sem,
    known_sem,
):
    devices, quarter, freqs, lons, lats = sizes
    consts = freq_constants(freqs)
    me = lax.axis_index("gx")
    east = lax.rem(me + 1, devices)
    west = lax.rem(me + devices - 1, devices)

    def load(k):
        return pltpu.make_async_copy(spectrum.at[:, k], buf.at[:, k], load_sem.at[k])

    for k in range(quarter):
        load(k).start()
    small = [
        pltpu.make_async_copy(wind, wind_v, small_sem.at[0]),
        pltpu.make_async_copy(land, land_v, small_sem.at[1]),
        pltpu.make_async_copy(band, band_v, small_sem.at[2]),
    ]
    for copy in small:
        copy.start()

    barrier = pltpu.get_barrier_semaphore()
    for neighbour in (west, east):
        pl.semaphore_signal(barrier, inc=1, device_id={"gx": neighbour}, device_id_type=MESH)

    for k in range(quarter):
        angle = (k + 0.5) * 2.0 * math.pi / (4 * quarter)
        trig[k] = jnp.float32(math.cos(angle))
        trig[quarter + k] = jnp.float32(math.sin(angle))
    rows = lax.broadcasted_iota(jnp.int32, (lons, lats), 0)
    lanes = lax.broadcasted_iota(jnp.int32, (lons, lats), 1)
    first_row = rows == 0
    last_row = rows == lons - 1
    inner_south = jnp.where(lanes == 0, 0.0, 1.0)
    inner_north = jnp.where(lanes == lats - 1, 0.0, 1.0)
    stokes_c[...] = jnp.zeros_like(stokes_c)
    stokes_s[...] = jnp.zeros_like(stokes_s)
    turned[...] = jnp.zeros_like(turned)

    for copy in small:
        copy.wait()
    mask = land_v[...].astype(jnp.float32)
    wind_east = wind_v[0]
    wind_north = wind_v[1]

    pl.semaphore_wait(barrier, 2)

    def tell(n):
        reach = 2**n
        for other in (lax.rem(me + reach, devices), lax.rem(me + devices - reach, devices)):
            pl.semaphore_signal(known_sem.at[n], inc=1, device_id={"gx": other}, device_id_type=MESH)

    def hear(n):
        pl.semaphore_wait(known_sem.at[n], 2)

    rounds = int(math.log2(devices)) - 1
    tell(0)

    def halo_copy(s, k, to_east):
        src, dst, side, where = (send_e, recv_e, 0, east) if to_east else (send_w, recv_w, 1, west)
        return pltpu.make_async_remote_copy(
            src_ref=src.at[s, k],
            dst_ref=dst.at[s, k],
            send_sem=halo_send_sem.at[s, side, k],
            recv_sem=halo_recv_sem.at[s, side, k],
            device_id={"gx": where},
            device_id_type=MESH,
        )

    def edge_copy(s, to_east):
        side, where = (0, east) if to_east else (1, west)
        return pltpu.make_async_remote_copy(
            src_ref=edge_send.at[s, side],
            dst_ref=edge_recv.at[s, side],
            send_sem=edge_send_sem.at[s, side],
            recv_sem=edge_recv_sem.at[s, side],
            device_id={"gx": where},
            device_id_type=MESH,
        )

    def pack(s, k):
        last = pl.ds(lons - 1, freqs, stride=lons)
        first = pl.ds(0, freqs, stride=lons)
        send_e[s, k, :freqs] = buf[0, k, last]
        send_e[s, k, freqs:] = buf[3, k, last]
        send_w[s, k, :freqs] = buf[1, k, first]
        send_w[s, k, freqs:] = buf[2, k, first]

    def ship(s, k):
        halo_copy(s, k, True).start()
        halo_copy(s, k, False).start()

    @pl.loop(0, quarter)
    def _(k):
        load(k).wait()
        pack(0, k)
        ship(0, k)

    def one_step(s):
        def body(k, carry):
            energy, across, along = carry
            c = jnp.full((lons, lats), trig[k], jnp.float32)
            n = jnp.full((lons, lats), trig[quarter + k], jnp.float32)
            both = c + n
            c_south, n_south = c * inner_south, n * inner_south
            c_north, n_north = c * inner_north, n * inner_north
            halo_copy(s, k, True).wait_recv()
            halo_copy(s, k, False).wait_recv()
            for heard, (at_step, at) in enumerate(HEARD):
                if at_step == s and heard + 1 < rounds:

                    @pl.when(k == at)
                    def _(heard=heard):
                        hear(heard)
                        tell(heard + 1)

            if s > 0:
                from_west = damp_edge[0]
                from_east = damp_edge[1]
                halo[0, :freqs] = recv_e[s, k, :freqs] * from_west
                halo[0, freqs:] = recv_e[s, k, freqs:] * from_west
                halo[1, :freqs] = recv_w[s, k, :freqs] * from_east
                halo[1, freqs:] = recv_w[s, k, freqs:] * from_east
            else:
                blow = wind_east * c + wind_north * n
                cross = wind_north * c - wind_east * n
            sum_across = jnp.zeros((lons, lats), jnp.float32)
            sum_along = jnp.zeros((lons, lats), jnp.float32)
            energy = list(energy)
            for j in range(freqs):
                shrink, speed, weight, _ = consts[j]
                tile = pl.ds(j * lons, lons)
                if s > 0:
                    d = damp[tile]
                if s == 0:
                    ahead = blow * speed
                    aside = cross * speed
                    gains = (ahead - 0.05, aside - 0.05, -0.05 - ahead, -0.05 - aside)
                new, flux = [], []
                for q in range(4):
                    center = buf[q, k, tile]
                    if s > 0:
                        center = center * d
                    eastward = q in (0, 3)
                    southern = q < 2
                    row = j + (freqs if q in (2, 3) else 0)
                    if s > 0:
                        edge = halo[0 if eastward else 1, pl.ds(row, 1)]
                    else:
                        edge = (recv_e if eastward else recv_w)[s, k, pl.ds(row, 1)]
                    if eastward:
                        upwind_x = jnp.where(first_row, edge, pltpu.roll(center, 1, 0))
                    else:
                        upwind_x = jnp.where(last_row, edge, pltpu.roll(center, lons - 1, 0))
                    upwind_y = pltpu.roll(center, 1 if southern else lats - 1, 1)
                    c_in, n_in = (c_south, n_south) if southern else (c_north, n_north)
                    x_rate, y_rate = (c, n_in) if q in (0, 2) else (n, c_in)
                    moved = center - shrink * (both * center - x_rate * upwind_x - y_rate * upwind_y)
                    energy[q] = energy[q] + moved
                    if s == 0:
                        gain = mask * jnp.minimum(jnp.maximum(gains[q], 0.0), 0.2)
                        grow[q, k, tile] = gain
                        gain_one = gain + mask
                        grow_one[q, k, tile] = gain_one
                    else:
                        gain_one = grow_one[q, k, tile]
                    value = moved * gain_one
                    buf[q, k, tile] = value
                    if s == STEPS - 1:
                        new.append(value)
                        flux.append(moved * grow[q, k, tile])
                if s == STEPS - 1:
                    sum_across = sum_across + weight * (flux[0] - flux[2])
                    sum_along = sum_along + weight * (flux[1] - flux[3])
                    d02 = new[0] - new[2]
                    d13 = new[1] - new[3]
                    stokes_c[tile] = stokes_c[tile] + (c * d02 - n * d13)
                    stokes_s[tile] = stokes_s[tile] + (n * d02 + c * d13)
            across = across + (c * sum_across - n * sum_along)
            along = along + (n * sum_across + c * sum_along)
            if s < STEPS - 1:
                pack(s + 1, k)

                @pl.when(k < EARLY)
                def _():
                    ship(s + 1, k)

            return tuple(energy), across, along

        zero = jnp.zeros((lons, lats), jnp.float32)
        energy, across, along = lax.fori_loop(0, quarter, body, ((zero,) * 4, zero, zero))
        total = (energy[0] + energy[1]) + (energy[2] + energy[3])
        return mask * total * (1.0 / (4 * quarter * freqs)), across, along

    def set_damping(energy):
        ratio = energy / (0.5 + energy)
        for j in range(freqs):
            damp[pl.ds(j * lons, lons)] = 1.0 / (1.0 + consts[j][3] * ratio)

    edge_weight = (lax.broadcasted_iota(jnp.int32, (freqs, lats), 0).astype(jnp.float32) + 1.0) / freqs
    edge_weight = 0.3 * edge_weight * edge_weight

    for s in range(STEPS):
        energy, across, along = one_step(s)
        if s < STEPS - 1:
            edge_send[s, 0] = energy[lons - 1 :]
            edge_send[s, 1] = energy[:1]
            edge_copy(s, True).start()
            edge_copy(s, False).start()
            for k in range(EARLY, quarter):
                ship(s + 1, k)
        set_damping(energy)
        if s == 0:
            lat = lax.broadcasted_iota(jnp.int32, (lats, lats), 0)
            place[...] = jnp.where(band_v[...] == lat, 1.0, 0.0).T
        if s < STEPS - 1:
            for side, to_east in ((0, True), (1, False)):
                edge_copy(s, to_east).wait_recv()
                other = edge_recv[s, side]
                ratio = other / (0.5 + other)
                damp_edge[side] = 1.0 / (1.0 + edge_weight * ratio)

    factor = 3.0 / math.sqrt(4 * quarter * freqs)
    drift_c = jnp.zeros((lons, lats), jnp.float32)
    drift_s = jnp.zeros((lons, lats), jnp.float32)
    for j in range(freqs):
        tile = pl.ds(j * lons, lons)
        d = damp[tile] * consts[j][2]
        drift_c = drift_c + d * stokes_c[tile]
        drift_s = drift_s + d * stokes_s[tile]
    parts = 4 * lons
    for c, value in enumerate((across, along, drift_c, drift_s)):
        value = factor * value
        turned[pl.ds(c * lons, lons), :lats] = value
        turned[pl.ds(parts + c * lons, lons), lats:] = value
    pick = jnp.concatenate(
        [place[pl.ds(0, devices, stride=2)], place[pl.ds(1, devices, stride=2)]], axis=1
    )
    message[:, 0, :] = lax.dot_general(
        pick,
        turned[...],
        (((1,), (1,)), ((), ())),
        precision=lax.Precision.HIGHEST,
        preferred_element_type=jnp.float32,
    )

    hear(rounds - 1)

    def message_copy(offset):
        to = lax.rem(me + offset, devices)
        return pltpu.make_async_remote_copy(
            src_ref=message.at[to],
            dst_ref=arrived.at[me],
            send_sem=message_send_sem,
            recv_sem=message_recv_sem,
            device_id={"gx": to},
            device_id_type=MESH,
        )

    half = devices // 2
    message_copy(half).start()

    @pl.loop(1, half)
    def _(near):
        message_copy(half - near).start()
        message_copy(half + near).start()

    arrived[me] = message[me]

    @pl.loop(0, quarter)
    def _(k):
        for j in range(freqs):
            tile = pl.ds(j * lons, lons)
            d = damp[tile]
            for q in range(4):
                buf[q, k, tile] = buf[q, k, tile] * d

    for s in range(STEPS):
        for k in range(quarter):
            halo_copy(s, k, True).wait_send()
            halo_copy(s, k, False).wait_send()
    for s in range(STEPS - 1):
        edge_copy(s, True).wait_send()
        edge_copy(s, False).wait_send()
    all_out = pltpu.make_async_remote_copy(
        src_ref=message.at[pl.ds(0, devices - 1)],
        dst_ref=arrived.at[pl.ds(0, devices - 1)],
        send_sem=message_send_sem,
        recv_sem=message_recv_sem,
        device_id={"gx": east},
        device_id_type=MESH,
    )
    all_out.wait_send()
    all_out.wait_recv()


def output_kernel(sizes, spectrum, arrived, spectrum_out, ocean_out, ocean, store_sem, ocean_sem):
    devices, lons, lats = sizes
    stores = [
        pltpu.make_async_copy(spectrum.at[q], spectrum_out.at[q], store_sem.at[q]) for q in range(4)
    ]
    for copy in stores:
        copy.start()
    rows = lax.broadcasted_iota(jnp.int32, (8, lats), 0)
    block = lax.broadcasted_iota(jnp.int32, (8, lats), 1) // lons
    per = lats // lons
    ahead = lax.rem(block - rows + per, per)
    wanted = [ahead == n for n in range(per)]
    for b in range(devices // per):
        pieces = []
        for h in range(per // 8):
            piece = arrived[pl.ds(b * per + h * 8, 8), 0, :]
            pieces.append(pltpu.roll(piece, h * 8 * lons, 1, stride=lons, stride_axis=0))
        for slot in range(8):
            total = jnp.zeros((8, lats), jnp.float32)
            for h, piece in enumerate(pieces):
                total = total + jnp.where(wanted[(slot + h * 8) % per], piece, 0.0)
            line = jnp.sum(total, axis=0, keepdims=True)
            if slot:
                line = pltpu.roll(jnp.broadcast_to(line, (8, lats)), lats - slot * lons, 1)[:1]
            r, c = divmod(slot, 4)
            ocean[c, pl.ds(r, 1), pl.ds(b * lats, lats)] = line
    last = pltpu.make_async_copy(ocean, ocean_out, ocean_sem)
    last.start()
    last.wait()
    for copy in stores:
        copy.wait()


def solution(mesh):
    devices = mesh.shape["gx"]

    def per_device(spectrum, wind, land_sea, band_rows):
        dirs, freqs, lons, lats = spectrum.shape
        quarter = dirs // 4
        tiles = freqs * lons
        f32 = jnp.float32
        hbm_space = pl.BlockSpec(memory_space=pltpu.HBM)
        vmem_space = pl.BlockSpec(memory_space=pltpu.VMEM)
        dma = pltpu.SemaphoreType.DMA
        final, arrived = pl.pallas_call(
            functools.partial(window_kernel, (devices, quarter, freqs, lons, lats)),
            out_shape=(
                pltpu.VMEM((4, quarter, tiles, lats), f32),
                pltpu.VMEM((devices, 1, lats), f32),
            ),
            in_specs=[hbm_space] * 4,
            out_specs=(vmem_space, vmem_space),
            scratch_shapes=[
                pltpu.VMEM((4, quarter, tiles, lats), f32),
                pltpu.VMEM((4, quarter, tiles, lats), f32),
                pltpu.VMEM((2, lons, lats), f32),
                pltpu.VMEM((lons, lats), jnp.int32),
                pltpu.VMEM((1, lats), jnp.int32),
                pltpu.SMEM((2 * quarter,), f32),
                pltpu.VMEM((STEPS, quarter, 2 * freqs, lats), f32),
                pltpu.VMEM((STEPS, quarter, 2 * freqs, lats), f32),
                pltpu.VMEM((STEPS, quarter, 2 * freqs, lats), f32),
                pltpu.VMEM((STEPS, quarter, 2 * freqs, lats), f32),
                pltpu.VMEM((2, 2 * freqs, lats), f32),
                pltpu.VMEM((tiles, lats), f32),
                pltpu.VMEM((2, freqs, lats), f32),
                pltpu.VMEM((STEPS - 1, 2, 1, lats), f32),
                pltpu.VMEM((STEPS - 1, 2, 1, lats), f32),
                pltpu.VMEM((tiles, lats), f32),
                pltpu.VMEM((tiles, lats), f32),
                pltpu.VMEM((lats, lats), f32),
                pltpu.VMEM((lats, 2 * lats), f32),
                pltpu.VMEM((devices, 1, lats), f32),
                dma((quarter,)),
                dma((3,)),
                dma((STEPS, 2, quarter)),
                dma((STEPS, 2, quarter)),
                dma((STEPS - 1, 2)),
                dma((STEPS - 1, 2)),
                dma,
                dma,
                pltpu.SemaphoreType.REGULAR((5,)),
            ],
            compiler_params=pltpu.CompilerParams(
                collective_id=0, has_side_effects=True, vmem_limit_bytes=KERNEL_VMEM
            ),
        )(
            *(
                pltpu.with_memory_space_constraint(argument, pltpu.HBM)
                for argument in (
                    spectrum.reshape(4, quarter, tiles, lats),
                    wind,
                    land_sea,
                    band_rows.reshape(1, lats),
                )
            )
        )
        next_spectrum, ocean = pl.pallas_call(
            functools.partial(output_kernel, (devices, lons, lats)),
            out_shape=(
                jax.ShapeDtypeStruct((4, quarter, tiles, lats), f32),
                jax.ShapeDtypeStruct((4, 2, devices * lons), f32),
            ),
            in_specs=[vmem_space] * 2,
            out_specs=(hbm_space, hbm_space),
            scratch_shapes=[
                pltpu.VMEM((4, 2, devices * lons), f32),
                dma((4,)),
                dma,
            ],
            compiler_params=pltpu.CompilerParams(vmem_limit_bytes=KERNEL_VMEM),
        )(final, arrived)
        return next_spectrum.reshape(spectrum.shape), ocean

    return jax.shard_map(
        per_device,
        mesh=mesh,
        in_specs=(P(None, None, MEMBER_GX, None), P(None, MEMBER_GX, None), P("gx", None), P(None)),
        out_specs=(P(None, None, MEMBER_GX, None), P(None, "gx", "member")),
        check_vma=False,
    )
```

```python
import functools
import math

import jax
import jax.numpy as jnp
from jax import lax
from jax.experimental import pallas as pl
from jax.experimental.pallas import tpu as pltpu
from jax.sharding import PartitionSpec as P

STEPS = 3
EARLY = (5, 4)
AHEAD = (5, 6, 6)
KERNEL_VMEM = 36 * 2**20
HEARD = ((-1, 0), (-1, 0), (0, 6), (1, 1))
MEMBER_GX = ("member", "gx")
MESH = pl.DeviceIdType.MESH


def freq_constants(freqs):
    out = []
    for j in range(freqs):
        shrink = 1.1 ** (-j)
        weight = (j + 1) / freqs
        inverse_speed = 2.0 * math.pi * (0.0418 / shrink) / 9.81
        out.append((0.45 * shrink, 0.05 * inverse_speed, weight, 0.3 * weight * weight))
    return out


def window_kernel(
    sizes,
    spectrum,
    wind,
    land,
    band,
    buf,
    arrived,
    grow,
    grow_one,
    wind_v,
    land_v,
    band_v,
    trig,
    send_e,
    send_w,
    recv_e,
    recv_w,
    halo,
    damp,
    damp_edge,
    shrink_rows,
    edge_send,
    edge_recv,
    stokes_c,
    stokes_s,
    place,
    turned,
    message,
    load_sem,
    small_sem,
    halo_send_sem,
    halo_recv_sem,
    edge_send_sem,
    edge_recv_sem,
    message_send_sem,
    message_recv_sem,
    known_sem,
):
    devices, quarter, freqs, lons, lats = sizes
    consts = freq_constants(freqs)
    me = lax.axis_index("gx")
    east = lax.rem(me + 1, devices)
    west = lax.rem(me + devices - 1, devices)

    def load(k):
        return pltpu.make_async_copy(spectrum.at[:, k], buf.at[:, k], load_sem.at[k])

    for k in range(quarter):
        load(k).start()
    small = [
        pltpu.make_async_copy(wind, wind_v, small_sem.at[0]),
        pltpu.make_async_copy(land, land_v, small_sem.at[1]),
        pltpu.make_async_copy(band, band_v, small_sem.at[2]),
    ]
    for copy in small:
        copy.start()

    barrier = pltpu.get_barrier_semaphore()
    for neighbour in (west, east):
        pl.semaphore_signal(barrier, inc=1, device_id={"gx": neighbour}, device_id_type=MESH)

    for k in range(quarter):
        angle = (k + 0.5) * 2.0 * math.pi / (4 * quarter)
        trig[k] = jnp.float32(math.cos(angle))
        trig[quarter + k] = jnp.float32(math.sin(angle))
    rows = lax.broadcasted_iota(jnp.int32, (lons, lats), 0)
    lanes = lax.broadcasted_iota(jnp.int32, (lons, lats), 1)
    first_row = jnp.where(rows == 0, 1.0, 0.0)
    last_row = jnp.where(rows == lons - 1, 1.0, 0.0)
    inner_south = jnp.where(lanes == 0, 0.0, 1.0)
    inner_north = jnp.where(lanes == lats - 1, 0.0, 1.0)
    stokes_c[...] = jnp.zeros_like(stokes_c)
    stokes_s[...] = jnp.zeros_like(stokes_s)
    turned[...] = jnp.zeros_like(turned)
    for j in range(freqs):
        line = jnp.full((1, lats), consts[j][0], jnp.float32)
        for rows_of in (shrink_rows, damp_edge.at[0], damp_edge.at[1]):
            rows_of[pl.ds(j, 1)] = line

    with jax.named_scope("barrier_wait"):
        for copy in small:
            copy.wait()
        mask = land_v[...].astype(jnp.float32)
        wind_east = wind_v[0]
        wind_north = wind_v[1]

        pl.semaphore_wait(barrier, 2)

    def tell(n):
        reach = 2**n
        for other in (lax.rem(me + reach, devices), lax.rem(me + devices - reach, devices)):
            pl.semaphore_signal(known_sem.at[n], inc=1, device_id={"gx": other}, device_id_type=MESH)

    def hear(n):
        pl.semaphore_wait(known_sem.at[n], 2)

    rounds = int(math.log2(devices)) - 1
    tell(0)

    def halo_copy(s, k, to_east):
        src, dst, side, where = (send_e, recv_e, 0, east) if to_east else (send_w, recv_w, 1, west)
        return pltpu.make_async_remote_copy(
            src_ref=src.at[s, k],
            dst_ref=dst.at[s, k],
            send_sem=halo_send_sem.at[s, side, k],
            recv_sem=halo_recv_sem.at[s, side, k],
            device_id={"gx": where},
            device_id_type=MESH,
        )

    def edge_copy(s, to_east):
        side, where = (0, east) if to_east else (1, west)
        return pltpu.make_async_remote_copy(
            src_ref=edge_send.at[s, side],
            dst_ref=edge_recv.at[s, side],
            send_sem=edge_send_sem.at[s, side],
            recv_sem=edge_recv_sem.at[s, side],
            device_id={"gx": where},
            device_id_type=MESH,
        )

    def pack(s, k):
        last = pl.ds(lons - 1, freqs, stride=lons)
        first = pl.ds(0, freqs, stride=lons)
        send_e[s, k, :freqs] = buf[0, k, last]
        send_e[s, k, freqs:] = buf[3, k, last]
        send_w[s, k, :freqs] = buf[1, k, first]
        send_w[s, k, freqs:] = buf[2, k, first]

    def ship(s, k):
        halo_copy(s, k, True).start()
        halo_copy(s, k, False).start()

    with jax.named_scope("first_ship"):
        @pl.loop(0, quarter)
        def _(k):
            load(k).wait()
            pack(0, k)
            ship(0, k)

    def body(s, mode, k, carry):
        energy, across, along = carry
        c = jnp.full((lons, lats), trig[k], jnp.float32)
        n = jnp.full((lons, lats), trig[quarter + k], jnp.float32)
        both = c + n
        y_rates = ((n * inner_south, c * inner_south), (n * inner_north, c * inner_north))
        x_rates = (c, n, c, n)
        sides = (0, 1, 1, 0)
        if mode != "start":
            halo_copy(s, k, True).wait_recv()
            halo_copy(s, k, False).wait_recv()
            for heard, (at_step, at) in enumerate(HEARD):
                if at_step == s and heard + 1 < rounds:

                    @pl.when(k == at)
                    def _(heard=heard):
                        hear(heard)
                        tell(heard + 1)

            for side, got in ((0, recv_e), (1, recv_w)):
                scale = damp_edge[side]
                halo[side, :freqs] = got[s, k, :freqs] * scale
                halo[side, freqs:] = got[s, k, freqs:] * scale
            outer = [x_rates[q] * (first_row, last_row)[sides[q]] for q in range(4)]
        if mode != "finish":
            inner = [x_rates[q] * (1.0 - (first_row, last_row)[sides[q]]) for q in range(4)]
            if s == 0:
                blow = wind_east * c + wind_north * n
                cross = wind_north * c - wind_east * n
        sum_across = jnp.zeros((lons, lats), jnp.float32)
        sum_along = jnp.zeros((lons, lats), jnp.float32)
        energy = list(energy)
        for j in range(freqs):
            shrink, speed, weight, _ = consts[j]
            tile = pl.ds(j * lons, lons)
            if mode != "finish":
                if s > 0:
                    d = damp[tile]
                else:
                    ahead = blow * speed
                    aside = cross * speed
                    gains = (ahead - 0.05, aside - 0.05, -0.05 - ahead, -0.05 - aside)
            new, flux = [], []
            for q in range(4):
                if mode == "finish":
                    moved = buf[q, k, tile]
                else:
                    center = buf[q, k, tile]
                    if s > 0:
                        center = center * d
                    upwind_x = pltpu.roll(center, lons - 1 if sides[q] else 1, 0)
                    upwind_y = pltpu.roll(center, 1 if q < 2 else lats - 1, 1)
                    change = both * center - inner[q] * upwind_x - y_rates[q // 2][q % 2] * upwind_y
                    moved = center - shrink * change
                    if s == 0:
                        gain = mask * jnp.minimum(jnp.maximum(gains[q], 0.0), 0.2)
                        grow[q, k, tile] = gain
                        gain_one = gain + mask
                        grow_one[q, k, tile] = gain_one
                if mode == "start":
                    buf[q, k, tile] = moved
                    continue
                row = j + (freqs if q >= 2 else 0)
                moved = moved + outer[q] * halo[sides[q], pl.ds(row, 1)]
                energy[q] = energy[q] + moved
                if s > 0 or mode == "finish":
                    gain_one = grow_one[q, k, tile]
                value = moved * gain_one
                buf[q, k, tile] = value
                if s == STEPS - 1:
                    new.append(value)
                    flux.append(moved * grow[q, k, tile])
            if s == STEPS - 1 and mode != "start":
                sum_across = sum_across + weight * (flux[0] - flux[2])
                sum_along = sum_along + weight * (flux[1] - flux[3])
                d02 = new[0] - new[2]
                d13 = new[1] - new[3]
                stokes_c[tile] = stokes_c[tile] + (c * d02 - n * d13)
                stokes_s[tile] = stokes_s[tile] + (n * d02 + c * d13)
        if mode == "start":
            return carry
        across = across + (c * sum_across - n * sum_along)
        along = along + (n * sum_across + c * sum_along)
        if s < STEPS - 1:
            pack(s + 1, k)

            @pl.when(k < EARLY[s])
            def _():
                ship(s + 1, k)

        return tuple(energy), across, along

    zero = jnp.zeros((lons, lats), jnp.float32)
    nothing = ((zero,) * 4, zero, zero)

    def start_step(s):
        lax.fori_loop(0, AHEAD[s], functools.partial(body, s, "start"), nothing)

    def finish_step(s):
        carry = lax.fori_loop(0, AHEAD[s], functools.partial(body, s, "finish"), nothing)
        carry = lax.fori_loop(AHEAD[s], quarter, functools.partial(body, s, "full"), carry)
        energy, across, along = carry
        total = (energy[0] + energy[1]) + (energy[2] + energy[3])
        return mask * total * (1.0 / (4 * quarter * freqs)), across, along

    def set_damping(energy):
        ratio = energy / (0.5 + energy)
        for j in range(freqs):
            damp[pl.ds(j * lons, lons)] = 1.0 / (1.0 + consts[j][3] * ratio)

    with jax.named_scope("start0"):
        start_step(0)
    for heard in (0, 1):
        hear(heard)
        tell(heard + 1)
    edge_weight = (lax.broadcasted_iota(jnp.int32, (freqs, lats), 0).astype(jnp.float32) + 1.0) / freqs
    edge_weight = 0.3 * edge_weight * edge_weight

    for s in range(STEPS):
        with jax.named_scope(f"step{s}"):
            energy, across, along = finish_step(s)
        if s < STEPS - 1:
            edge_send[s, 0] = energy[lons - 1 :]
            edge_send[s, 1] = energy[:1]
            edge_copy(s, True).start()
            edge_copy(s, False).start()
            for k in range(EARLY[s], quarter):
                ship(s + 1, k)
        set_damping(energy)
        if s == 0:
            lat = lax.broadcasted_iota(jnp.int32, (lats, lats), 0)
            place[...] = jnp.where(band_v[...] == lat, 1.0, 0.0).T
        if s < STEPS - 1:
            with jax.named_scope(f"start{s + 1}"):
                start_step(s + 1)
            for side, to_east in ((0, True), (1, False)):
                with jax.named_scope(f"edge{s}{side}"):
                    edge_copy(s, to_east).wait_recv()
                other = edge_recv[s, side]
                ratio = other / (0.5 + other)
                damp_edge[side] = shrink_rows[...] / (1.0 + edge_weight * ratio)

    with jax.named_scope("fields"):
        factor = 3.0 / math.sqrt(4 * quarter * freqs)
        drift_c = jnp.zeros((lons, lats), jnp.float32)
        drift_s = jnp.zeros((lons, lats), jnp.float32)
        for j in range(freqs):
            tile = pl.ds(j * lons, lons)
            d = damp[tile] * consts[j][2]
            drift_c = drift_c + d * stokes_c[tile]
            drift_s = drift_s + d * stokes_s[tile]
        parts = 4 * lons
        for c, value in enumerate((across, along, drift_c, drift_s)):
            value = factor * value
            turned[pl.ds(c * lons, lons), :lats] = value
            turned[pl.ds(parts + c * lons, lons), lats:] = value
        pick = jnp.concatenate(
            [place[pl.ds(0, devices, stride=2)], place[pl.ds(1, devices, stride=2)]], axis=1
        )
        message[:, 0, :] = lax.dot_general(
            pick,
            turned[...],
            (((1,), (1,)), ((), ())),
            precision=lax.Precision.HIGHEST,
            preferred_element_type=jnp.float32,
        )

    with jax.named_scope("hear"):
        hear(rounds - 1)

    def message_copy(offset):
        to = lax.rem(me + offset, devices)
        return pltpu.make_async_remote_copy(
            src_ref=message.at[to],
            dst_ref=arrived.at[me],
            send_sem=message_send_sem,
            recv_sem=message_recv_sem,
            device_id={"gx": to},
            device_id_type=MESH,
        )

    with jax.named_scope("issue"):
        half = devices // 2
        message_copy(half).start()

        @pl.loop(1, half)
        def _(near):
            message_copy(half - near).start()
            message_copy(half + near).start()

    arrived[me] = message[me]

    @pl.loop(0, quarter)
    def _(k):
        for j in range(freqs):
            tile = pl.ds(j * lons, lons)
            d = damp[tile]
            for q in range(4):
                buf[q, k, tile] = buf[q, k, tile] * d

    for s in range(STEPS):
        for k in range(quarter):
            halo_copy(s, k, True).wait_send()
            halo_copy(s, k, False).wait_send()
    for s in range(STEPS - 1):
        edge_copy(s, True).wait_send()
        edge_copy(s, False).wait_send()
    all_out = pltpu.make_async_remote_copy(
        src_ref=message.at[pl.ds(0, devices - 1)],
        dst_ref=arrived.at[pl.ds(0, devices - 1)],
        send_sem=message_send_sem,
        recv_sem=message_recv_sem,
        device_id={"gx": east},
        device_id_type=MESH,
    )
    with jax.named_scope("wait_send"):
        all_out.wait_send()
    with jax.named_scope("wait_recv"):
        all_out.wait_recv()


def output_kernel(sizes, spectrum, arrived, spectrum_out, ocean_out, ocean, store_sem, ocean_sem):
    devices, lons, lats = sizes
    stores = [
        pltpu.make_async_copy(spectrum.at[q], spectrum_out.at[q], store_sem.at[q]) for q in range(4)
    ]
    for copy in stores:
        copy.start()
    rows = lax.broadcasted_iota(jnp.int32, (8, lats), 0)
    block = lax.broadcasted_iota(jnp.int32, (8, lats), 1) // lons
    per = lats // lons
    ahead = lax.rem(block - rows + per, per)
    wanted = [ahead == n for n in range(per)]
    for b in range(devices // per):
        pieces = []
        for h in range(per // 8):
            piece = arrived[pl.ds(b * per + h * 8, 8), 0, :]
            pieces.append(pltpu.roll(piece, h * 8 * lons, 1, stride=lons, stride_axis=0))
        for slot in range(8):
            total = jnp.zeros((8, lats), jnp.float32)
            for h, piece in enumerate(pieces):
                total = total + jnp.where(wanted[(slot + h * 8) % per], piece, 0.0)
            line = jnp.sum(total, axis=0, keepdims=True)
            if slot:
                line = pltpu.roll(jnp.broadcast_to(line, (8, lats)), lats - slot * lons, 1)[:1]
            r, c = divmod(slot, 4)
            ocean[c, pl.ds(r, 1), pl.ds(b * lats, lats)] = line
    last = pltpu.make_async_copy(ocean, ocean_out, ocean_sem)
    last.start()
    last.wait()
    for copy in stores:
        copy.wait()


def solution(mesh):
    devices = mesh.shape["gx"]

    def per_device(spectrum, wind, land_sea, band_rows):
        dirs, freqs, lons, lats = spectrum.shape
        quarter = dirs // 4
        tiles = freqs * lons
        f32 = jnp.float32
        hbm_space = pl.BlockSpec(memory_space=pltpu.HBM)
        vmem_space = pl.BlockSpec(memory_space=pltpu.VMEM)
        dma = pltpu.SemaphoreType.DMA
        final, arrived = pl.pallas_call(
            functools.partial(window_kernel, (devices, quarter, freqs, lons, lats)),
            out_shape=(
                pltpu.VMEM((4, quarter, tiles, lats), f32),
                pltpu.VMEM((devices, 1, lats), f32),
            ),
            in_specs=[hbm_space] * 4,
            out_specs=(vmem_space, vmem_space),
            scratch_shapes=[
                pltpu.VMEM((4, quarter, tiles, lats), f32),
                pltpu.VMEM((4, quarter, tiles, lats), f32),
                pltpu.VMEM((2, lons, lats), f32),
                pltpu.VMEM((lons, lats), jnp.int32),
                pltpu.VMEM((1, lats), jnp.int32),
                pltpu.SMEM((2 * quarter,), f32),
                pltpu.VMEM((STEPS, quarter, 2 * freqs, lats), f32),
                pltpu.VMEM((STEPS, quarter, 2 * freqs, lats), f32),
                pltpu.VMEM((STEPS, quarter, 2 * freqs, lats), f32),
                pltpu.VMEM((STEPS, quarter, 2 * freqs, lats), f32),
                pltpu.VMEM((2, 2 * freqs, lats), f32),
                pltpu.VMEM((tiles, lats), f32),
                pltpu.VMEM((2, freqs, lats), f32),
                pltpu.VMEM((freqs, lats), f32),
                pltpu.VMEM((STEPS - 1, 2, 1, lats), f32),
                pltpu.VMEM((STEPS - 1, 2, 1, lats), f32),
                pltpu.VMEM((tiles, lats), f32),
                pltpu.VMEM((tiles, lats), f32),
                pltpu.VMEM((lats, lats), f32),
                pltpu.VMEM((lats, 2 * lats), f32),
                pltpu.VMEM((devices, 1, lats), f32),
                dma((quarter,)),
                dma((3,)),
                dma((STEPS, 2, quarter)),
                dma((STEPS, 2, quarter)),
                dma((STEPS - 1, 2)),
                dma((STEPS - 1, 2)),
                dma,
                dma,
                pltpu.SemaphoreType.REGULAR((5,)),
            ],
            compiler_params=pltpu.CompilerParams(
                collective_id=0, has_side_effects=True, vmem_limit_bytes=KERNEL_VMEM
            ),
        )(
            *(
                pltpu.with_memory_space_constraint(argument, pltpu.HBM)
                for argument in (
                    spectrum.reshape(4, quarter, tiles, lats),
                    wind,
                    land_sea,
                    band_rows.reshape(1, lats),
                )
            )
        )
        next_spectrum, ocean = pl.pallas_call(
            functools.partial(output_kernel, (devices, lons, lats)),
            out_shape=(
                jax.ShapeDtypeStruct((4, quarter, tiles, lats), f32),
                jax.ShapeDtypeStruct((4, 2, devices * lons), f32),
            ),
            in_specs=[vmem_space] * 2,
            out_specs=(hbm_space, hbm_space),
            scratch_shapes=[
                pltpu.VMEM((4, 2, devices * lons), f32),
                dma((4,)),
                dma,
            ],
            compiler_params=pltpu.CompilerParams(vmem_limit_bytes=KERNEL_VMEM),
        )(final, arrived)
        return next_spectrum.reshape(spectrum.shape), ocean

    return jax.shard_map(
        per_device,
        mesh=mesh,
        in_specs=(P(None, None, MEMBER_GX, None), P(None, MEMBER_GX, None), P("gx", None), P(None)),
        out_specs=(P(None, None, MEMBER_GX, None), P(None, "gx", "member")),
        check_vma=False,
    )
```

```python
import functools
import math

import jax
import jax.numpy as jnp
from jax import lax
from jax.experimental import pallas as pl
from jax.experimental.pallas import tpu as pltpu
from jax.sharding import PartitionSpec as P

STEPS = 3
EARLY = (4, 4)
KERNEL_VMEM = 36 * 2**20
HEARD = 7
MEMBER_GX = ("member", "gx")
MESH = pl.DeviceIdType.MESH


def freq_constants(freqs):
    out = []
    for j in range(freqs):
        shrink = 1.1 ** (-j)
        weight = (j + 1) / freqs
        inverse_speed = 2.0 * math.pi * (0.0418 / shrink) / 9.81
        out.append((0.45 * shrink, 0.05 * inverse_speed, weight, 0.3 * weight * weight))
    return out


def window_kernel(
    sizes,
    spectrum,
    wind,
    land,
    band,
    buf,
    arrived,
    grow,
    grow_one,
    wind_v,
    land_v,
    band_v,
    trig,
    send_e,
    send_w,
    recv_e,
    recv_w,
    halo,
    damp,
    damp_edge,
    shrink_rows,
    edge_send,
    edge_recv,
    stokes_c,
    stokes_s,
    place,
    turned,
    message,
    load_sem,
    small_sem,
    halo_send_sem,
    halo_recv_sem,
    edge_send_sem,
    edge_recv_sem,
    message_send_sem,
    message_recv_sem,
    known_sem,
):
    devices, quarter, freqs, lons, lats = sizes
    consts = freq_constants(freqs)
    me = lax.axis_index("gx")
    east = lax.rem(me + 1, devices)
    west = lax.rem(me + devices - 1, devices)

    def load(k):
        return pltpu.make_async_copy(spectrum.at[:, k], buf.at[:, k], load_sem.at[k])

    for k in range(quarter):
        load(k).start()
    small = [
        pltpu.make_async_copy(wind, wind_v, small_sem.at[0]),
        pltpu.make_async_copy(land, land_v, small_sem.at[1]),
        pltpu.make_async_copy(band, band_v, small_sem.at[2]),
    ]
    for copy in small:
        copy.start()

    barrier = pltpu.get_barrier_semaphore()
    for neighbour in (west, east):
        pl.semaphore_signal(barrier, inc=1, device_id={"gx": neighbour}, device_id_type=MESH)

    for k in range(quarter):
        angle = (k + 0.5) * 2.0 * math.pi / (4 * quarter)
        trig[k] = jnp.float32(math.cos(angle))
        trig[quarter + k] = jnp.float32(math.sin(angle))
    rows = lax.broadcasted_iota(jnp.int32, (lons, lats), 0)
    lanes = lax.broadcasted_iota(jnp.int32, (lons, lats), 1)
    first_row = jnp.where(rows == 0, 1.0, 0.0)
    last_row = jnp.where(rows == lons - 1, 1.0, 0.0)
    inner_south = jnp.where(lanes == 0, 0.0, 1.0)
    inner_north = jnp.where(lanes == lats - 1, 0.0, 1.0)
    stokes_c[...] = jnp.zeros_like(stokes_c)
    stokes_s[...] = jnp.zeros_like(stokes_s)
    turned[...] = jnp.zeros_like(turned)
    for j in range(freqs):
        line = jnp.full((1, lats), consts[j][0], jnp.float32)
        for rows_of in (shrink_rows, damp_edge.at[0], damp_edge.at[1]):
            rows_of[pl.ds(j, 1)] = line

    with jax.named_scope("barrier_wait"):
        for copy in small:
            copy.wait()
        mask = land_v[...].astype(jnp.float32)
        wind_east = wind_v[0]
        wind_north = wind_v[1]

        pl.semaphore_wait(barrier, 2)

    def tell(n):
        reach = 2**n
        for other in (lax.rem(me + reach, devices), lax.rem(me + devices - reach, devices)):
            pl.semaphore_signal(known_sem.at[n], inc=1, device_id={"gx": other}, device_id_type=MESH)

    def hear(n):
        pl.semaphore_wait(known_sem.at[n], 2)

    rounds = 5
    assert 2 ** (rounds + 1) == devices
    tell(0)

    def halo_copy(s, k, to_east):
        src, dst, side, where = (send_e, recv_e, 0, east) if to_east else (send_w, recv_w, 1, west)
        return pltpu.make_async_remote_copy(
            src_ref=src.at[s, k],
            dst_ref=dst.at[s, k],
            send_sem=halo_send_sem.at[s, side, k],
            recv_sem=halo_recv_sem.at[s, side, k],
            device_id={"gx": where},
            device_id_type=MESH,
        )

    def edge_copy(s, to_east):
        side, where = (0, east) if to_east else (1, west)
        return pltpu.make_async_remote_copy(
            src_ref=edge_send.at[s, side],
            dst_ref=edge_recv.at[s, side],
            send_sem=edge_send_sem.at[s, side],
            recv_sem=edge_recv_sem.at[s, side],
            device_id={"gx": where},
            device_id_type=MESH,
        )

    def pack(s, k):
        last = pl.ds(lons - 1, freqs, stride=lons)
        first = pl.ds(0, freqs, stride=lons)
        send_e[s, k, :freqs] = buf[0, k, last]
        send_e[s, k, freqs:] = buf[3, k, last]
        send_w[s, k, :freqs] = buf[1, k, first]
        send_w[s, k, freqs:] = buf[2, k, first]

    def ship(s, k):
        halo_copy(s, k, True).start()
        halo_copy(s, k, False).start()

    with jax.named_scope("first_ship"):
        @pl.loop(0, quarter)
        def _(k):
            load(k).wait()
            pack(0, k)
            ship(0, k)

    def body(s, mode, k, carry):
        energy, across, along = carry
        c = jnp.full((lons, lats), trig[k], jnp.float32)
        n = jnp.full((lons, lats), trig[quarter + k], jnp.float32)
        both = c + n
        y_rates = ((n * inner_south, c * inner_south), (n * inner_north, c * inner_north))
        x_rates = (c, n, c, n)
        sides = (0, 1, 1, 0)
        if mode == "finish":
            halo_copy(s, k, True).wait_recv()
            halo_copy(s, k, False).wait_recv()
            if s == 0:

                @pl.when(k == HEARD)
                def _():
                    hear(2)
                    tell(3)

            for side, got in ((0, recv_e), (1, recv_w)):
                scale = damp_edge[side]
                halo[side, :freqs] = got[s, k, :freqs] * scale
                halo[side, freqs:] = got[s, k, freqs:] * scale
            outer = [x_rates[q] * (first_row, last_row)[sides[q]] for q in range(4)]
        else:
            inner = [x_rates[q] * (1.0 - (first_row, last_row)[sides[q]]) for q in range(4)]
            if s == 0:
                blow = wind_east * c + wind_north * n
                cross = wind_north * c - wind_east * n
        sum_across = jnp.zeros((lons, lats), jnp.float32)
        sum_along = jnp.zeros((lons, lats), jnp.float32)
        energy = list(energy)
        for j in range(freqs):
            shrink, speed, weight, _ = consts[j]
            tile = pl.ds(j * lons, lons)
            if mode != "finish":
                if s > 0:
                    d = damp[tile]
                else:
                    ahead = blow * speed
                    aside = cross * speed
                    gains = (ahead - 0.05, aside - 0.05, -0.05 - ahead, -0.05 - aside)
            new, flux = [], []
            for q in range(4):
                if mode == "finish":
                    moved = buf[q, k, tile]
                else:
                    center = buf[q, k, tile]
                    if s > 0:
                        center = center * d
                    upwind_x = pltpu.roll(center, lons - 1 if sides[q] else 1, 0)
                    upwind_y = pltpu.roll(center, 1 if q < 2 else lats - 1, 1)
                    change = both * center - inner[q] * upwind_x - y_rates[q // 2][q % 2] * upwind_y
                    moved = center - shrink * change
                    if s == 0:
                        gain = mask * jnp.minimum(jnp.maximum(gains[q], 0.0), 0.2)
                        grow[q, k, tile] = gain
                        gain_one = gain + mask
                        grow_one[q, k, tile] = gain_one
                if mode == "start":
                    buf[q, k, tile] = moved
                    continue
                row = j + (freqs if q >= 2 else 0)
                moved = moved + outer[q] * halo[sides[q], pl.ds(row, 1)]
                energy[q] = energy[q] + moved
                value = moved * grow_one[q, k, tile]
                buf[q, k, tile] = value
                if s == STEPS - 1:
                    new.append(value)
                    flux.append(moved * grow[q, k, tile])
            if s == STEPS - 1 and mode == "finish":
                sum_across = sum_across + weight * (flux[0] - flux[2])
                sum_along = sum_along + weight * (flux[1] - flux[3])
                d02 = new[0] - new[2]
                d13 = new[1] - new[3]
                stokes_c[tile] = stokes_c[tile] + (c * d02 - n * d13)
                stokes_s[tile] = stokes_s[tile] + (n * d02 + c * d13)
        if mode == "start":
            return carry
        across = across + (c * sum_across - n * sum_along)
        along = along + (n * sum_across + c * sum_along)
        if s < STEPS - 1:
            pack(s + 1, k)

            @pl.when(k < EARLY[s])
            def _():
                ship(s + 1, k)

        return tuple(energy), across, along

    zero = jnp.zeros((lons, lats), jnp.float32)
    nothing = ((zero,) * 4, zero, zero)

    def start_step(s):
        lax.fori_loop(0, quarter, functools.partial(body, s, "start"), nothing)

    def finish_step(s):
        energy, across, along = lax.fori_loop(
            0, quarter, functools.partial(body, s, "finish"), nothing
        )
        total = (energy[0] + energy[1]) + (energy[2] + energy[3])
        return mask * total * (1.0 / (4 * quarter * freqs)), across, along

    def set_damping(energy):
        ratio = energy / (0.5 + energy)
        for j in range(freqs):
            damp[pl.ds(j * lons, lons)] = 1.0 / (1.0 + consts[j][3] * ratio)

    hear(0)
    tell(1)
    with jax.named_scope("start0"):
        start_step(0)
    hear(1)
    tell(2)
    edge_weight = (lax.broadcasted_iota(jnp.int32, (freqs, lats), 0).astype(jnp.float32) + 1.0) / freqs
    edge_weight = 0.3 * edge_weight * edge_weight

    for s in range(STEPS):
        with jax.named_scope(f"step{s}"):
            energy, across, along = finish_step(s)
        if s < STEPS - 1:
            edge_send[s, 0] = energy[lons - 1 :]
            edge_send[s, 1] = energy[:1]
            edge_copy(s, True).start()
            edge_copy(s, False).start()
            for k in range(EARLY[s], quarter):
                ship(s + 1, k)
        set_damping(energy)
        if s == 0:
            lat = lax.broadcasted_iota(jnp.int32, (lats, lats), 0)
            place[...] = jnp.where(band_v[...] == lat, 1.0, 0.0).T
        if s < STEPS - 1:
            with jax.named_scope(f"start{s + 1}"):
                start_step(s + 1)
            if s == 0:
                hear(3)
                tell(4)
            for side, to_east in ((0, True), (1, False)):
                with jax.named_scope(f"edge{s}{side}"):
                    edge_copy(s, to_east).wait_recv()
                other = edge_recv[s, side]
                ratio = other / (0.5 + other)
                damp_edge[side] = shrink_rows[...] / (1.0 + edge_weight * ratio)

    with jax.named_scope("fields"):
        factor = 3.0 / math.sqrt(4 * quarter * freqs)
        drift_c = jnp.zeros((lons, lats), jnp.float32)
        drift_s = jnp.zeros((lons, lats), jnp.float32)
        for j in range(freqs):
            tile = pl.ds(j * lons, lons)
            d = damp[tile] * consts[j][2]
            drift_c = drift_c + d * stokes_c[tile]
            drift_s = drift_s + d * stokes_s[tile]
        parts = 4 * lons
        for c, value in enumerate((across, along, drift_c, drift_s)):
            value = factor * value
            turned[pl.ds(c * lons, lons), :lats] = value
            turned[pl.ds(parts + c * lons, lons), lats:] = value
        pick = jnp.concatenate(
            [place[pl.ds(0, devices, stride=2)], place[pl.ds(1, devices, stride=2)]], axis=1
        )
        message[:, 0, :] = lax.dot_general(
            pick,
            turned[...],
            (((1,), (1,)), ((), ())),
            precision=lax.Precision.HIGHEST,
            preferred_element_type=jnp.float32,
        )

    with jax.named_scope("hear"):
        hear(rounds - 1)

    def message_copy(offset):
        to = lax.rem(me + offset, devices)
        return pltpu.make_async_remote_copy(
            src_ref=message.at[to],
            dst_ref=arrived.at[me],
            send_sem=message_send_sem,
            recv_sem=message_recv_sem,
            device_id={"gx": to},
            device_id_type=MESH,
        )

    with jax.named_scope("issue"):
        half = devices // 2
        message_copy(half).start()

        @pl.loop(1, half)
        def _(near):
            message_copy(half - near).start()
            message_copy(half + near).start()

    arrived[me] = message[me]

    @pl.loop(0, quarter)
    def _(k):
        for j in range(freqs):
            tile = pl.ds(j * lons, lons)
            d = damp[tile]
            for q in range(4):
                buf[q, k, tile] = buf[q, k, tile] * d

    for s in range(STEPS):
        for k in range(quarter):
            halo_copy(s, k, True).wait_send()
            halo_copy(s, k, False).wait_send()
    for s in range(STEPS - 1):
        edge_copy(s, True).wait_send()
        edge_copy(s, False).wait_send()
    all_out = pltpu.make_async_remote_copy(
        src_ref=message.at[pl.ds(0, devices - 1)],
        dst_ref=arrived.at[pl.ds(0, devices - 1)],
        send_sem=message_send_sem,
        recv_sem=message_recv_sem,
        device_id={"gx": east},
        device_id_type=MESH,
    )
    with jax.named_scope("wait_send"):
        all_out.wait_send()
    with jax.named_scope("wait_recv"):
        all_out.wait_recv()


def output_kernel(sizes, spectrum, arrived, spectrum_out, ocean_out, ocean, store_sem, ocean_sem):
    devices, lons, lats = sizes
    stores = [
        pltpu.make_async_copy(spectrum.at[q], spectrum_out.at[q], store_sem.at[q]) for q in range(4)
    ]
    for copy in stores:
        copy.start()
    rows = lax.broadcasted_iota(jnp.int32, (8, lats), 0)
    block = lax.broadcasted_iota(jnp.int32, (8, lats), 1) // lons
    per = lats // lons
    ahead = lax.rem(block - rows + per, per)
    wanted = [ahead == n for n in range(per)]
    for b in range(devices // per):
        pieces = []
        for h in range(per // 8):
            piece = arrived[pl.ds(b * per + h * 8, 8), 0, :]
            pieces.append(pltpu.roll(piece, h * 8 * lons, 1, stride=lons, stride_axis=0))
        for slot in range(8):
            total = jnp.zeros((8, lats), jnp.float32)
            for h, piece in enumerate(pieces):
                total = total + jnp.where(wanted[(slot + h * 8) % per], piece, 0.0)
            line = jnp.sum(total, axis=0, keepdims=True)
            if slot:
                line = pltpu.roll(jnp.broadcast_to(line, (8, lats)), lats - slot * lons, 1)[:1]
            r, c = divmod(slot, 4)
            ocean[c, pl.ds(r, 1), pl.ds(b * lats, lats)] = line
    last = pltpu.make_async_copy(ocean, ocean_out, ocean_sem)
    last.start()
    last.wait()
    for copy in stores:
        copy.wait()


def solution(mesh):
    devices = mesh.shape["gx"]

    def per_device(spectrum, wind, land_sea, band_rows):
        dirs, freqs, lons, lats = spectrum.shape
        quarter = dirs // 4
        tiles = freqs * lons
        f32 = jnp.float32
        hbm_space = pl.BlockSpec(memory_space=pltpu.HBM)
        vmem_space = pl.BlockSpec(memory_space=pltpu.VMEM)
        dma = pltpu.SemaphoreType.DMA
        final, arrived = pl.pallas_call(
            functools.partial(window_kernel, (devices, quarter, freqs, lons, lats)),
            out_shape=(
                pltpu.VMEM((4, quarter, tiles, lats), f32),
                pltpu.VMEM((devices, 1, lats), f32),
            ),
            in_specs=[hbm_space] * 4,
            out_specs=(vmem_space, vmem_space),
            scratch_shapes=[
                pltpu.VMEM((4, quarter, tiles, lats), f32),
                pltpu.VMEM((4, quarter, tiles, lats), f32),
                pltpu.VMEM((2, lons, lats), f32),
                pltpu.VMEM((lons, lats), jnp.int32),
                pltpu.VMEM((1, lats), jnp.int32),
                pltpu.SMEM((2 * quarter,), f32),
                pltpu.VMEM((STEPS, quarter, 2 * freqs, lats), f32),
                pltpu.VMEM((STEPS, quarter, 2 * freqs, lats), f32),
                pltpu.VMEM((STEPS, quarter, 2 * freqs, lats), f32),
                pltpu.VMEM((STEPS, quarter, 2 * freqs, lats), f32),
                pltpu.VMEM((2, 2 * freqs, lats), f32),
                pltpu.VMEM((tiles, lats), f32),
                pltpu.VMEM((2, freqs, lats), f32),
                pltpu.VMEM((freqs, lats), f32),
                pltpu.VMEM((STEPS - 1, 2, 1, lats), f32),
                pltpu.VMEM((STEPS - 1, 2, 1, lats), f32),
                pltpu.VMEM((tiles, lats), f32),
                pltpu.VMEM((tiles, lats), f32),
                pltpu.VMEM((lats, lats), f32),
                pltpu.VMEM((lats, 2 * lats), f32),
                pltpu.VMEM((devices, 1, lats), f32),
                dma((quarter,)),
                dma((3,)),
                dma((STEPS, 2, quarter)),
                dma((STEPS, 2, quarter)),
                dma((STEPS - 1, 2)),
                dma((STEPS - 1, 2)),
                dma,
                dma,
                pltpu.SemaphoreType.REGULAR((5,)),
            ],
            compiler_params=pltpu.CompilerParams(
                collective_id=0, has_side_effects=True, vmem_limit_bytes=KERNEL_VMEM
            ),
        )(
            *(
                pltpu.with_memory_space_constraint(argument, pltpu.HBM)
                for argument in (
                    spectrum.reshape(4, quarter, tiles, lats),
                    wind,
                    land_sea,
                    band_rows.reshape(1, lats),
                )
            )
        )
        next_spectrum, ocean = pl.pallas_call(
            functools.partial(output_kernel, (devices, lons, lats)),
            out_shape=(
                jax.ShapeDtypeStruct((4, quarter, tiles, lats), f32),
                jax.ShapeDtypeStruct((4, 2, devices * lons), f32),
            ),
            in_specs=[vmem_space] * 2,
            out_specs=(hbm_space, hbm_space),
            scratch_shapes=[
                pltpu.VMEM((4, 2, devices * lons), f32),
                dma((4,)),
                dma,
            ],
            compiler_params=pltpu.CompilerParams(vmem_limit_bytes=KERNEL_VMEM),
        )(final, arrived)
        return next_spectrum.reshape(spectrum.shape), ocean

    return jax.shard_map(
        per_device,
        mesh=mesh,
        in_specs=(P(None, None, MEMBER_GX, None), P(None, MEMBER_GX, None), P("gx", None), P(None)),
        out_specs=(P(None, None, MEMBER_GX, None), P(None, "gx", "member")),
        check_vma=False,
    )
```

```python
import functools
import math

import jax
import jax.numpy as jnp
from jax import lax
from jax.experimental import pallas as pl
from jax.experimental.pallas import tpu as pltpu
from jax.sharding import PartitionSpec as P

STEPS = 3
EARLY = (5, 5)
KERNEL_VMEM = 36 * 2**20
HEARD = ((0, 3), (0, 9), (0, 6), (1, 2))
MEMBER_GX = ("member", "gx")
MESH = pl.DeviceIdType.MESH


def freq_constants(freqs):
    out = []
    for j in range(freqs):
        shrink = 1.1 ** (-j)
        weight = (j + 1) / freqs
        inverse_speed = 2.0 * math.pi * (0.0418 / shrink) / 9.81
        out.append((0.45 * shrink, 0.05 * inverse_speed, weight, 0.3 * weight * weight))
    return out


def window_kernel(
    sizes,
    spectrum,
    wind,
    land,
    band,
    buf,
    arrived,
    grow,
    grow_one,
    wind_v,
    land_v,
    band_v,
    trig,
    send_e,
    send_w,
    recv_e,
    recv_w,
    halo,
    damp,
    damp_edge,
    shrink_rows,
    edge_send,
    edge_recv,
    stokes_c,
    stokes_s,
    place,
    turned,
    message,
    load_sem,
    small_sem,
    halo_send_sem,
    halo_recv_sem,
    edge_send_sem,
    edge_recv_sem,
    message_send_sem,
    message_recv_sem,
    known_sem,
):
    devices, quarter, freqs, lons, lats = sizes
    consts = freq_constants(freqs)
    me = lax.axis_index("gx")
    east = lax.rem(me + 1, devices)
    west = lax.rem(me + devices - 1, devices)

    barrier = pltpu.get_barrier_semaphore()
    for neighbour in (west, east):
        pl.semaphore_signal(barrier, inc=1, device_id={"gx": neighbour}, device_id_type=MESH)

    def load(k):
        return pltpu.make_async_copy(spectrum.at[:, k], buf.at[:, k], load_sem.at[k])

    small = [
        pltpu.make_async_copy(wind, wind_v, small_sem.at[0]),
        pltpu.make_async_copy(land, land_v, small_sem.at[1]),
        pltpu.make_async_copy(band, band_v, small_sem.at[2]),
    ]
    for copy in small:
        copy.start()

    for k in range(quarter):
        load(k).start()

    for k in range(quarter):
        angle = (k + 0.5) * 2.0 * math.pi / (4 * quarter)
        trig[k] = jnp.float32(math.cos(angle))
        trig[quarter + k] = jnp.float32(math.sin(angle))
    rows = lax.broadcasted_iota(jnp.int32, (lons, lats), 0)
    lanes = lax.broadcasted_iota(jnp.int32, (lons, lats), 1)
    first_row = jnp.where(rows == 0, 1.0, 0.0)
    last_row = jnp.where(rows == lons - 1, 1.0, 0.0)
    inner_south = jnp.where(lanes == 0, 0.0, 1.0)
    inner_north = jnp.where(lanes == lats - 1, 0.0, 1.0)
    stokes_c[...] = jnp.zeros_like(stokes_c)
    stokes_s[...] = jnp.zeros_like(stokes_s)
    turned[...] = jnp.zeros_like(turned)
    for j in range(freqs):
        line = jnp.full((1, lats), consts[j][0], jnp.float32)
        for rows_of in (shrink_rows, damp_edge.at[0], damp_edge.at[1]):
            rows_of[pl.ds(j, 1)] = line

    with jax.named_scope("barrier_wait"):
        pl.semaphore_wait(barrier, 2)

    def tell(n):
        reach = 2**n
        for other in (lax.rem(me + reach, devices), lax.rem(me + devices - reach, devices)):
            pl.semaphore_signal(known_sem.at[n], inc=1, device_id={"gx": other}, device_id_type=MESH)

    def hear(n):
        pl.semaphore_wait(known_sem.at[n], 2)

    rounds = 5
    assert 2 ** (rounds + 1) == devices
    tell(0)

    def halo_copy(s, k, to_east):
        src, dst, side, where = (send_e, recv_e, 0, east) if to_east else (send_w, recv_w, 1, west)
        return pltpu.make_async_remote_copy(
            src_ref=src.at[s, k],
            dst_ref=dst.at[s, k],
            send_sem=halo_send_sem.at[s, side, k],
            recv_sem=halo_recv_sem.at[s, side, k],
            device_id={"gx": where},
            device_id_type=MESH,
        )

    def edge_copy(s, to_east):
        side, where = (0, east) if to_east else (1, west)
        return pltpu.make_async_remote_copy(
            src_ref=edge_send.at[s, side],
            dst_ref=edge_recv.at[s, side],
            send_sem=edge_send_sem.at[s, side],
            recv_sem=edge_recv_sem.at[s, side],
            device_id={"gx": where},
            device_id_type=MESH,
        )

    def pack(s, k):
        last = pl.ds(lons - 1, freqs, stride=lons)
        first = pl.ds(0, freqs, stride=lons)
        send_e[s, k, :freqs] = buf[0, k, last]
        send_e[s, k, freqs:] = buf[3, k, last]
        send_w[s, k, :freqs] = buf[1, k, first]
        send_w[s, k, freqs:] = buf[2, k, first]

    def ship(s, k):
        halo_copy(s, k, True).start()
        halo_copy(s, k, False).start()

    with jax.named_scope("first_ship"):
        @pl.loop(0, quarter)
        def _(k):
            load(k).wait()
            pack(0, k)
            ship(0, k)

    for copy in small:
        copy.wait()
    mask = land_v[...].astype(jnp.float32)
    wind_east = wind_v[0]
    wind_north = wind_v[1]

    def body(s, mode, k, carry):
        energy, across, along = carry
        c = jnp.full((lons, lats), trig[k], jnp.float32)
        n = jnp.full((lons, lats), trig[quarter + k], jnp.float32)
        both = c + n
        y_rates = ((n * inner_south, c * inner_south), (n * inner_north, c * inner_north))
        x_rates = (c, n, c, n)
        sides = (0, 1, 1, 0)
        if mode == "finish":
            halo_copy(s, k, True).wait_recv()
            halo_copy(s, k, False).wait_recv()
            for heard in (2, 3):
                if HEARD[heard][0] == s:

                    @pl.when(k == HEARD[heard][1])
                    def _(heard=heard):
                        hear(heard)
                        tell(heard + 1)

            for side, got in ((0, recv_e), (1, recv_w)):
                scale = damp_edge[side]
                halo[side, :freqs] = got[s, k, :freqs] * scale
                halo[side, freqs:] = got[s, k, freqs:] * scale
            outer = [x_rates[q] * (first_row, last_row)[sides[q]] for q in range(4)]
        else:
            inner = [x_rates[q] * (1.0 - (first_row, last_row)[sides[q]]) for q in range(4)]
            if s == 0:

                @pl.when(k == HEARD[0][1])
                def _():
                    hear(0)
                    tell(1)

                blow = wind_east * c + wind_north * n
                cross = wind_north * c - wind_east * n
        sum_across = jnp.zeros((lons, lats), jnp.float32)
        sum_along = jnp.zeros((lons, lats), jnp.float32)
        energy = list(energy)
        for j in range(freqs):
            shrink, speed, weight, _ = consts[j]
            tile = pl.ds(j * lons, lons)
            if mode != "finish":
                if s > 0:
                    d = damp[tile]
                else:
                    ahead = blow * speed
                    aside = cross * speed
                    gains = (ahead - 0.05, aside - 0.05, -0.05 - ahead, -0.05 - aside)
            new, flux = [], []
            for q in range(4):
                if mode == "finish":
                    moved = buf[q, k, tile]
                else:
                    center = buf[q, k, tile]
                    if s > 0:
                        center = center * d
                    upwind_x = pltpu.roll(center, lons - 1 if sides[q] else 1, 0)
                    upwind_y = pltpu.roll(center, 1 if q < 2 else lats - 1, 1)
                    change = both * center - inner[q] * upwind_x - y_rates[q // 2][q % 2] * upwind_y
                    moved = center - shrink * change
                    if s == 0:
                        gain = mask * jnp.minimum(jnp.maximum(gains[q], 0.0), 0.2)
                        grow[q, k, tile] = gain
                        gain_one = gain + mask
                        grow_one[q, k, tile] = gain_one
                if mode == "start":
                    buf[q, k, tile] = moved
                    continue
                row = j + (freqs if q >= 2 else 0)
                moved = moved + outer[q] * halo[sides[q], pl.ds(row, 1)]
                energy[q] = energy[q] + moved
                value = moved * grow_one[q, k, tile]
                buf[q, k, tile] = value
                if s == STEPS - 1:
                    new.append(value)
                    flux.append(moved * grow[q, k, tile])
            if s == STEPS - 1 and mode == "finish":
                sum_across = sum_across + weight * (flux[0] - flux[2])
                sum_along = sum_along + weight * (flux[1] - flux[3])
                d02 = new[0] - new[2]
                d13 = new[1] - new[3]
                stokes_c[tile] = stokes_c[tile] + (c * d02 - n * d13)
                stokes_s[tile] = stokes_s[tile] + (n * d02 + c * d13)
        if mode == "start":
            return carry
        across = across + (c * sum_across - n * sum_along)
        along = along + (n * sum_across + c * sum_along)
        if s < STEPS - 1:
            pack(s + 1, k)

            @pl.when(k < EARLY[s])
            def _():
                ship(s + 1, k)

        return tuple(energy), across, along

    zero = jnp.zeros((lons, lats), jnp.float32)
    nothing = ((zero,) * 4, zero, zero)

    def start_step(s):
        lax.fori_loop(0, quarter, functools.partial(body, s, "start"), nothing)

    def finish_step(s):
        energy, across, along = lax.fori_loop(
            0, quarter, functools.partial(body, s, "finish"), nothing
        )
        total = (energy[0] + energy[1]) + (energy[2] + energy[3])
        return mask * total * (1.0 / (4 * quarter * freqs)), across, along

    def set_damping(energy):
        ratio = energy / (0.5 + energy)
        for j in range(freqs):
            damp[pl.ds(j * lons, lons)] = 1.0 / (1.0 + consts[j][3] * ratio)

    with jax.named_scope("start0"):
        start_step(0)
    hear(1)
    tell(2)
    edge_weight = (lax.broadcasted_iota(jnp.int32, (freqs, lats), 0).astype(jnp.float32) + 1.0) / freqs
    edge_weight = 0.3 * edge_weight * edge_weight

    for s in range(STEPS):
        with jax.named_scope(f"step{s}"):
            energy, across, along = finish_step(s)
        if s < STEPS - 1:
            edge_send[s, 0] = energy[lons - 1 :]
            edge_send[s, 1] = energy[:1]
            edge_copy(s, True).start()
            edge_copy(s, False).start()
            for k in range(EARLY[s], quarter):
                ship(s + 1, k)
        set_damping(energy)
        if s == 0:
            lat = lax.broadcasted_iota(jnp.int32, (lats, lats), 0)
            place[...] = jnp.where(band_v[...] == lat, 1.0, 0.0).T
        if s < STEPS - 1:
            with jax.named_scope(f"start{s + 1}"):
                start_step(s + 1)
            for side, to_east in ((0, True), (1, False)):
                with jax.named_scope(f"edge{s}{side}"):
                    edge_copy(s, to_east).wait_recv()
                other = edge_recv[s, side]
                ratio = other / (0.5 + other)
                damp_edge[side] = shrink_rows[...] / (1.0 + edge_weight * ratio)

    with jax.named_scope("fields"):
        factor = 3.0 / math.sqrt(4 * quarter * freqs)
        drift_c = jnp.zeros((lons, lats), jnp.float32)
        drift_s = jnp.zeros((lons, lats), jnp.float32)
        for j in range(freqs):
            tile = pl.ds(j * lons, lons)
            d = damp[tile] * consts[j][2]
            drift_c = drift_c + d * stokes_c[tile]
            drift_s = drift_s + d * stokes_s[tile]
        parts = 4 * lons
        for c, value in enumerate((across, along, drift_c, drift_s)):
            value = factor * value
            turned[pl.ds(c * lons, lons), :lats] = value
            turned[pl.ds(parts + c * lons, lons), lats:] = value
        pick = jnp.concatenate(
            [place[pl.ds(0, devices, stride=2)], place[pl.ds(1, devices, stride=2)]], axis=1
        )
        message[:, 0, :] = lax.dot_general(
            pick,
            turned[...],
            (((1,), (1,)), ((), ())),
            precision=lax.Precision.HIGHEST,
            preferred_element_type=jnp.float32,
        )

    with jax.named_scope("hear"):
        hear(rounds - 1)

    def message_copy(offset):
        to = lax.rem(me + offset, devices)
        return pltpu.make_async_remote_copy(
            src_ref=message.at[to],
            dst_ref=arrived.at[me],
            send_sem=message_send_sem,
            recv_sem=message_recv_sem,
            device_id={"gx": to},
            device_id_type=MESH,
        )

    with jax.named_scope("issue"):
        half = devices // 2
        message_copy(half).start()

        @pl.loop(1, half)
        def _(near):
            message_copy(half - near).start()
            message_copy(half + near).start()

    arrived[me] = message[me]

    @pl.loop(0, quarter)
    def _(k):
        for j in range(freqs):
            tile = pl.ds(j * lons, lons)
            d = damp[tile]
            for q in range(4):
                buf[q, k, tile] = buf[q, k, tile] * d

    for s in range(STEPS):
        for k in range(quarter):
            halo_copy(s, k, True).wait_send()
            halo_copy(s, k, False).wait_send()
    for s in range(STEPS - 1):
        edge_copy(s, True).wait_send()
        edge_copy(s, False).wait_send()
    all_out = pltpu.make_async_remote_copy(
        src_ref=message.at[pl.ds(0, devices - 1)],
        dst_ref=arrived.at[pl.ds(0, devices - 1)],
        send_sem=message_send_sem,
        recv_sem=message_recv_sem,
        device_id={"gx": east},
        device_id_type=MESH,
    )
    with jax.named_scope("wait_send"):
        all_out.wait_send()
    with jax.named_scope("wait_recv"):
        all_out.wait_recv()


def output_kernel(sizes, spectrum, arrived, spectrum_out, ocean_out, ocean, store_sem, ocean_sem):
    devices, lons, lats = sizes
    stores = [
        pltpu.make_async_copy(spectrum.at[q], spectrum_out.at[q], store_sem.at[q]) for q in range(4)
    ]
    for copy in stores:
        copy.start()
    rows = lax.broadcasted_iota(jnp.int32, (8, lats), 0)
    block = lax.broadcasted_iota(jnp.int32, (8, lats), 1) // lons
    per = lats // lons
    ahead = lax.rem(block - rows + per, per)
    wanted = [ahead == n for n in range(per)]
    for b in range(devices // per):
        pieces = []
        for h in range(per // 8):
            piece = arrived[pl.ds(b * per + h * 8, 8), 0, :]
            pieces.append(pltpu.roll(piece, h * 8 * lons, 1, stride=lons, stride_axis=0))
        for slot in range(8):
            total = jnp.zeros((8, lats), jnp.float32)
            for h, piece in enumerate(pieces):
                total = total + jnp.where(wanted[(slot + h * 8) % per], piece, 0.0)
            line = jnp.sum(total, axis=0, keepdims=True)
            if slot:
                line = pltpu.roll(jnp.broadcast_to(line, (8, lats)), lats - slot * lons, 1)[:1]
            r, c = divmod(slot, 4)
            ocean[c, pl.ds(r, 1), pl.ds(b * lats, lats)] = line
    last = pltpu.make_async_copy(ocean, ocean_out, ocean_sem)
    last.start()
    last.wait()
    for copy in stores:
        copy.wait()


def solution(mesh):
    devices = mesh.shape["gx"]

    def per_device(spectrum, wind, land_sea, band_rows):
        dirs, freqs, lons, lats = spectrum.shape
        quarter = dirs // 4
        tiles = freqs * lons
        f32 = jnp.float32
        hbm_space = pl.BlockSpec(memory_space=pltpu.HBM)
        vmem_space = pl.BlockSpec(memory_space=pltpu.VMEM)
        dma = pltpu.SemaphoreType.DMA
        final, arrived = pl.pallas_call(
            functools.partial(window_kernel, (devices, quarter, freqs, lons, lats)),
            out_shape=(
                pltpu.VMEM((4, quarter, tiles, lats), f32),
                pltpu.VMEM((devices, 1, lats), f32),
            ),
            in_specs=[hbm_space] * 4,
            out_specs=(vmem_space, vmem_space),
            scratch_shapes=[
                pltpu.VMEM((4, quarter, tiles, lats), f32),
                pltpu.VMEM((4, quarter, tiles, lats), f32),
                pltpu.VMEM((2, lons, lats), f32),
                pltpu.VMEM((lons, lats), jnp.int32),
                pltpu.VMEM((1, lats), jnp.int32),
                pltpu.SMEM((2 * quarter,), f32),
                pltpu.VMEM((STEPS, quarter, 2 * freqs, lats), f32),
                pltpu.VMEM((STEPS, quarter, 2 * freqs, lats), f32),
                pltpu.VMEM((STEPS, quarter, 2 * freqs, lats), f32),
                pltpu.VMEM((STEPS, quarter, 2 * freqs, lats), f32),
                pltpu.VMEM((2, 2 * freqs, lats), f32),
                pltpu.VMEM((tiles, lats), f32),
                pltpu.VMEM((2, freqs, lats), f32),
                pltpu.VMEM((freqs, lats), f32),
                pltpu.VMEM((STEPS - 1, 2, 1, lats), f32),
                pltpu.VMEM((STEPS - 1, 2, 1, lats), f32),
                pltpu.VMEM((tiles, lats), f32),
                pltpu.VMEM((tiles, lats), f32),
                pltpu.VMEM((lats, lats), f32),
                pltpu.VMEM((lats, 2 * lats), f32),
                pltpu.VMEM((devices, 1, lats), f32),
                dma((quarter,)),
                dma((3,)),
                dma((STEPS, 2, quarter)),
                dma((STEPS, 2, quarter)),
                dma((STEPS - 1, 2)),
                dma((STEPS - 1, 2)),
                dma,
                dma,
                pltpu.SemaphoreType.REGULAR((5,)),
            ],
            compiler_params=pltpu.CompilerParams(
                collective_id=0, has_side_effects=True, vmem_limit_bytes=KERNEL_VMEM
            ),
        )(
            *(
                pltpu.with_memory_space_constraint(argument, pltpu.HBM)
                for argument in (
                    spectrum.reshape(4, quarter, tiles, lats),
                    wind,
                    land_sea,
                    band_rows.reshape(1, lats),
                )
            )
        )
        next_spectrum, ocean = pl.pallas_call(
            functools.partial(output_kernel, (devices, lons, lats)),
            out_shape=(
                jax.ShapeDtypeStruct((4, quarter, tiles, lats), f32),
                jax.ShapeDtypeStruct((4, 2, devices * lons), f32),
            ),
            in_specs=[vmem_space] * 2,
            out_specs=(hbm_space, hbm_space),
            scratch_shapes=[
                pltpu.VMEM((4, 2, devices * lons), f32),
                dma((4,)),
                dma,
            ],
            compiler_params=pltpu.CompilerParams(vmem_limit_bytes=KERNEL_VMEM),
        )(final, arrived)
        return next_spectrum.reshape(spectrum.shape), ocean

    return jax.shard_map(
        per_device,
        mesh=mesh,
        in_specs=(P(None, None, MEMBER_GX, None), P(None, MEMBER_GX, None), P("gx", None), P(None)),
        out_specs=(P(None, None, MEMBER_GX, None), P(None, "gx", "member")),
        check_vma=False,
    )
```

```python
import functools
import math

import jax
import jax.numpy as jnp
from jax import lax
from jax.experimental import pallas as pl
from jax.experimental.pallas import tpu as pltpu
from jax.sharding import PartitionSpec as P

STEPS = 3
EARLY = (5, 4)
KERNEL_VMEM = 36 * 2**20
HEARD = ((0, 3), (0, 9), (0, 6), (1, 2))
MEMBER_GX = ("member", "gx")
MESH = pl.DeviceIdType.MESH


def freq_constants(freqs):
    out = []
    for j in range(freqs):
        shrink = 1.1 ** (-j)
        weight = (j + 1) / freqs
        inverse_speed = 2.0 * math.pi * (0.0418 / shrink) / 9.81
        out.append((0.45 * shrink, 0.05 * inverse_speed, weight, 0.3 * weight * weight))
    return out


def window_kernel(
    sizes,
    spectrum,
    wind,
    land,
    band,
    buf,
    arrived,
    grow,
    grow_one,
    wind_v,
    land_v,
    band_v,
    trig,
    send_e,
    send_w,
    recv_e,
    recv_w,
    halo,
    damp,
    damp_edge,
    shrink_rows,
    edge_send,
    edge_recv,
    stokes_c,
    stokes_s,
    place,
    turned,
    message,
    load_sem,
    small_sem,
    halo_send_sem,
    halo_recv_sem,
    edge_send_sem,
    edge_recv_sem,
    message_send_sem,
    message_recv_sem,
    known_sem,
):
    devices, quarter, freqs, lons, lats = sizes
    consts = freq_constants(freqs)
    me = lax.axis_index("gx")
    east = lax.rem(me + 1, devices)
    west = lax.rem(me + devices - 1, devices)

    barrier = pltpu.get_barrier_semaphore()
    for neighbour in (west, east):
        pl.semaphore_signal(barrier, inc=1, device_id={"gx": neighbour}, device_id_type=MESH)

    def load(k):
        return pltpu.make_async_copy(spectrum.at[:, k], buf.at[:, k], load_sem.at[k])

    small = [
        pltpu.make_async_copy(wind, wind_v, small_sem.at[0]),
        pltpu.make_async_copy(land, land_v, small_sem.at[1]),
        pltpu.make_async_copy(band, band_v, small_sem.at[2]),
    ]
    for copy in small:
        copy.start()

    for k in range(quarter):
        load(k).start()

    for k in range(quarter):
        angle = (k + 0.5) * 2.0 * math.pi / (4 * quarter)
        trig[k] = jnp.float32(math.cos(angle))
        trig[quarter + k] = jnp.float32(math.sin(angle))
    rows = lax.broadcasted_iota(jnp.int32, (lons, lats), 0)
    lanes = lax.broadcasted_iota(jnp.int32, (lons, lats), 1)
    first_row = jnp.where(rows == 0, 1.0, 0.0)
    last_row = jnp.where(rows == lons - 1, 1.0, 0.0)
    inner_south = jnp.where(lanes == 0, 0.0, 1.0)
    inner_north = jnp.where(lanes == lats - 1, 0.0, 1.0)
    stokes_c[...] = jnp.zeros_like(stokes_c)
    stokes_s[...] = jnp.zeros_like(stokes_s)
    turned[...] = jnp.zeros_like(turned)
    for j in range(freqs):
        line = jnp.full((1, lats), consts[j][0], jnp.float32)
        for rows_of in (shrink_rows, damp_edge.at[0], damp_edge.at[1]):
            rows_of[pl.ds(j, 1)] = line

    with jax.named_scope("barrier_wait"):
        pl.semaphore_wait(barrier, 2)

    def tell(n):
        reach = 2**n
        for other in (lax.rem(me + reach, devices), lax.rem(me + devices - reach, devices)):
            pl.semaphore_signal(known_sem.at[n], inc=1, device_id={"gx": other}, device_id_type=MESH)

    def hear(n):
        pl.semaphore_wait(known_sem.at[n], 2)

    rounds = 5
    assert 2 ** (rounds + 1) == devices
    tell(0)

    def halo_copy(s, k, to_east):
        src, dst, side, where = (send_e, recv_e, 0, east) if to_east else (send_w, recv_w, 1, west)
        return pltpu.make_async_remote_copy(
            src_ref=src.at[s, k],
            dst_ref=dst.at[s, k],
            send_sem=halo_send_sem.at[s, side, k],
            recv_sem=halo_recv_sem.at[s, side, k],
            device_id={"gx": where},
            device_id_type=MESH,
        )

    def edge_copy(s, to_east):
        side, where = (0, east) if to_east else (1, west)
        return pltpu.make_async_remote_copy(
            src_ref=edge_send.at[s, side],
            dst_ref=edge_recv.at[s, side],
            send_sem=edge_send_sem.at[s, side],
            recv_sem=edge_recv_sem.at[s, side],
            device_id={"gx": where},
            device_id_type=MESH,
        )

    def pack(s, k):
        last = pl.ds(lons - 1, freqs, stride=lons)
        first = pl.ds(0, freqs, stride=lons)
        send_e[s, k, :freqs] = buf[0, k, last]
        send_e[s, k, freqs:] = buf[3, k, last]
        send_w[s, k, :freqs] = buf[1, k, first]
        send_w[s, k, freqs:] = buf[2, k, first]

    def ship(s, k):
        halo_copy(s, k, True).start()
        halo_copy(s, k, False).start()

    with jax.named_scope("first_ship"):
        @pl.loop(0, quarter)
        def _(k):
            load(k).wait()
            pack(0, k)
            ship(0, k)

    for copy in small:
        copy.wait()
    mask = land_v[...].astype(jnp.float32)
    wind_east = wind_v[0]
    wind_north = wind_v[1]

    def body(s, mode, k, carry):
        energy, across, along = carry
        c = jnp.full((lons, lats), trig[k], jnp.float32)
        n = jnp.full((lons, lats), trig[quarter + k], jnp.float32)
        both = c + n
        y_rates = ((n * inner_south, c * inner_south), (n * inner_north, c * inner_north))
        x_rates = (c, n, c, n)
        sides = (0, 1, 1, 0)
        if mode == "finish":
            halo_copy(s, k, True).wait_recv()
            halo_copy(s, k, False).wait_recv()
            for heard in (2, 3):
                if HEARD[heard][0] == s:

                    @pl.when(k == HEARD[heard][1])
                    def _(heard=heard):
                        hear(heard)
                        tell(heard + 1)

            for side, got in ((0, recv_e), (1, recv_w)):
                scale = damp_edge[side]
                halo[side, :freqs] = got[s, k, :freqs] * scale
                halo[side, freqs:] = got[s, k, freqs:] * scale
            outer = [x_rates[q] * (first_row, last_row)[sides[q]] for q in range(4)]
        else:
            inner = [x_rates[q] * (1.0 - (first_row, last_row)[sides[q]]) for q in range(4)]
            if s == 0:

                @pl.when(k == HEARD[0][1])
                def _():
                    hear(0)
                    tell(1)

                blow = wind_east * c + wind_north * n
                cross = wind_north * c - wind_east * n
        sum_across = jnp.zeros((lons, lats), jnp.float32)
        sum_along = jnp.zeros((lons, lats), jnp.float32)
        energy = list(energy)
        for j in range(freqs):
            shrink, speed, weight, _ = consts[j]
            tile = pl.ds(j * lons, lons)
            if mode != "finish":
                if s > 0:
                    d = damp[tile]
                else:
                    ahead = blow * speed
                    aside = cross * speed
                    gains = (ahead - 0.05, aside - 0.05, -0.05 - ahead, -0.05 - aside)
            new, flux = [], []
            for q in range(4):
                if mode == "finish":
                    moved = buf[q, k, tile]
                else:
                    center = buf[q, k, tile]
                    if s > 0:
                        center = center * d
                    upwind_x = pltpu.roll(center, lons - 1 if sides[q] else 1, 0)
                    upwind_y = pltpu.roll(center, 1 if q < 2 else lats - 1, 1)
                    change = both * center - inner[q] * upwind_x - y_rates[q // 2][q % 2] * upwind_y
                    moved = center - shrink * change
                    if s == 0:
                        gain = mask * jnp.minimum(jnp.maximum(gains[q], 0.0), 0.2)
                        grow[q, k, tile] = gain
                        gain_one = gain + mask
                        grow_one[q, k, tile] = gain_one
                if mode == "start":
                    buf[q, k, tile] = moved
                    continue
                row = j + (freqs if q >= 2 else 0)
                moved = moved + outer[q] * halo[sides[q], pl.ds(row, 1)]
                energy[q] = energy[q] + moved
                value = moved * grow_one[q, k, tile]
                buf[q, k, tile] = value
                if s == STEPS - 1:
                    new.append(value)
                    flux.append(moved * grow[q, k, tile])
            if s == STEPS - 1 and mode == "finish":
                sum_across = sum_across + weight * (flux[0] - flux[2])
                sum_along = sum_along + weight * (flux[1] - flux[3])
                d02 = new[0] - new[2]
                d13 = new[1] - new[3]
                stokes_c[tile] = stokes_c[tile] + (c * d02 - n * d13)
                stokes_s[tile] = stokes_s[tile] + (n * d02 + c * d13)
        if mode == "start":
            return carry
        across = across + (c * sum_across - n * sum_along)
        along = along + (n * sum_across + c * sum_along)
        if s < STEPS - 1:
            pack(s + 1, k)

            @pl.when(k < EARLY[s])
            def _():
                ship(s + 1, k)

        return tuple(energy), across, along

    zero = jnp.zeros((lons, lats), jnp.float32)
    nothing = ((zero,) * 4, zero, zero)

    def start_step(s):
        lax.fori_loop(0, quarter, functools.partial(body, s, "start"), nothing)

    def finish_step(s):
        energy, across, along = lax.fori_loop(
            0, quarter, functools.partial(body, s, "finish"), nothing
        )
        total = (energy[0] + energy[1]) + (energy[2] + energy[3])
        return mask * total * (1.0 / (4 * quarter * freqs)), across, along

    def set_damping(energy):
        ratio = energy / (0.5 + energy)
        for j in range(freqs):
            damp[pl.ds(j * lons, lons)] = 1.0 / (1.0 + consts[j][3] * ratio)

    with jax.named_scope("start0"):
        start_step(0)
    hear(1)
    tell(2)
    edge_weight = (lax.broadcasted_iota(jnp.int32, (freqs, lats), 0).astype(jnp.float32) + 1.0) / freqs
    edge_weight = 0.3 * edge_weight * edge_weight

    for s in range(STEPS):
        with jax.named_scope(f"step{s}"):
            energy, across, along = finish_step(s)
        if s < STEPS - 1:
            edge_send[s, 0] = energy[lons - 1 :]
            edge_send[s, 1] = energy[:1]
            edge_copy(s, True).start()
            edge_copy(s, False).start()
            for k in range(EARLY[s], quarter):
                ship(s + 1, k)
        set_damping(energy)
        if s == 0:
            lat = lax.broadcasted_iota(jnp.int32, (lats, lats), 0)
            place[...] = jnp.where(band_v[...] == lat, 1.0, 0.0).T
        if s < STEPS - 1:
            with jax.named_scope(f"start{s + 1}"):
                start_step(s + 1)
            for side, to_east in ((0, True), (1, False)):
                with jax.named_scope(f"edge{s}{side}"):
                    edge_copy(s, to_east).wait_recv()
                other = edge_recv[s, side]
                ratio = other / (0.5 + other)
                damp_edge[side] = shrink_rows[...] / (1.0 + edge_weight * ratio)

    with jax.named_scope("fields"):
        factor = 3.0 / math.sqrt(4 * quarter * freqs)
        drift_c = jnp.zeros((lons, lats), jnp.float32)
        drift_s = jnp.zeros((lons, lats), jnp.float32)
        for j in range(freqs):
            tile = pl.ds(j * lons, lons)
            d = damp[tile] * consts[j][2]
            drift_c = drift_c + d * stokes_c[tile]
            drift_s = drift_s + d * stokes_s[tile]
        parts = 4 * lons
        for c, value in enumerate((across, along, drift_c, drift_s)):
            value = factor * value
            turned[pl.ds(c * lons, lons), :lats] = value
            turned[pl.ds(parts + c * lons, lons), lats:] = value
        pick = jnp.concatenate(
            [place[pl.ds(0, devices, stride=2)], place[pl.ds(1, devices, stride=2)]], axis=1
        )
        message[:, 0, :] = lax.dot_general(
            pick,
            turned[...],
            (((1,), (1,)), ((), ())),
            precision=lax.Precision.HIGHEST,
            preferred_element_type=jnp.float32,
        )

    with jax.named_scope("hear"):
        hear(rounds - 1)

    def message_copy(offset):
        to = lax.rem(me + offset, devices)
        return pltpu.make_async_remote_copy(
            src_ref=message.at[to],
            dst_ref=arrived.at[me],
            send_sem=message_send_sem,
            recv_sem=message_recv_sem,
            device_id={"gx": to},
            device_id_type=MESH,
        )

    with jax.named_scope("issue"):
        half = devices // 2
        message_copy(half).start()

        @pl.loop(1, half)
        def _(near):
            message_copy(half - near).start()
            message_copy(half + near).start()

    arrived[me] = message[me]

    @pl.loop(0, quarter)
    def _(k):
        for j in range(freqs):
            tile = pl.ds(j * lons, lons)
            d = damp[tile]
            for q in range(4):
                buf[q, k, tile] = buf[q, k, tile] * d

    for s in range(STEPS):
        for k in range(quarter):
            halo_copy(s, k, True).wait_send()
            halo_copy(s, k, False).wait_send()
    for s in range(STEPS - 1):
        edge_copy(s, True).wait_send()
        edge_copy(s, False).wait_send()
    all_out = pltpu.make_async_remote_copy(
        src_ref=message.at[pl.ds(0, devices - 1)],
        dst_ref=arrived.at[pl.ds(0, devices - 1)],
        send_sem=message_send_sem,
        recv_sem=message_recv_sem,
        device_id={"gx": east},
        device_id_type=MESH,
    )
    with jax.named_scope("wait_send"):
        all_out.wait_send()
    with jax.named_scope("wait_recv"):
        all_out.wait_recv()


def output_kernel(sizes, spectrum, arrived, spectrum_out, ocean_out, ocean, store_sem, ocean_sem):
    devices, lons, lats = sizes
    stores = [
        pltpu.make_async_copy(spectrum.at[q], spectrum_out.at[q], store_sem.at[q]) for q in range(4)
    ]
    for copy in stores:
        copy.start()
    rows = lax.broadcasted_iota(jnp.int32, (8, lats), 0)
    block = lax.broadcasted_iota(jnp.int32, (8, lats), 1) // lons
    per = lats // lons
    ahead = lax.rem(block - rows + per, per)
    wanted = [ahead == n for n in range(per)]
    for b in range(devices // per):
        pieces = []
        for h in range(per // 8):
            piece = arrived[pl.ds(b * per + h * 8, 8), 0, :]
            pieces.append(pltpu.roll(piece, h * 8 * lons, 1, stride=lons, stride_axis=0))
        for slot in range(8):
            total = jnp.zeros((8, lats), jnp.float32)
            for h, piece in enumerate(pieces):
                total = total + jnp.where(wanted[(slot + h * 8) % per], piece, 0.0)
            line = jnp.sum(total, axis=0, keepdims=True)
            if slot:
                line = pltpu.roll(jnp.broadcast_to(line, (8, lats)), lats - slot * lons, 1)[:1]
            r, c = divmod(slot, 4)
            ocean[c, pl.ds(r, 1), pl.ds(b * lats, lats)] = line
    last = pltpu.make_async_copy(ocean, ocean_out, ocean_sem)
    last.start()
    last.wait()
    for copy in stores:
        copy.wait()


def solution(mesh):
    devices = mesh.shape["gx"]

    def per_device(spectrum, wind, land_sea, band_rows):
        dirs, freqs, lons, lats = spectrum.shape
        quarter = dirs // 4
        tiles = freqs * lons
        f32 = jnp.float32
        hbm_space = pl.BlockSpec(memory_space=pltpu.HBM)
        vmem_space = pl.BlockSpec(memory_space=pltpu.VMEM)
        dma = pltpu.SemaphoreType.DMA
        final, arrived = pl.pallas_call(
            functools.partial(window_kernel, (devices, quarter, freqs, lons, lats)),
            out_shape=(
                pltpu.VMEM((4, quarter, tiles, lats), f32),
                pltpu.VMEM((devices, 1, lats), f32),
            ),
            in_specs=[hbm_space] * 4,
            out_specs=(vmem_space, vmem_space),
            scratch_shapes=[
                pltpu.VMEM((4, quarter, tiles, lats), f32),
                pltpu.VMEM((4, quarter, tiles, lats), f32),
                pltpu.VMEM((2, lons, lats), f32),
                pltpu.VMEM((lons, lats), jnp.int32),
                pltpu.VMEM((1, lats), jnp.int32),
                pltpu.SMEM((2 * quarter,), f32),
                pltpu.VMEM((STEPS, quarter, 2 * freqs, lats), f32),
                pltpu.VMEM((STEPS, quarter, 2 * freqs, lats), f32),
                pltpu.VMEM((STEPS, quarter, 2 * freqs, lats), f32),
                pltpu.VMEM((STEPS, quarter, 2 * freqs, lats), f32),
                pltpu.VMEM((2, 2 * freqs, lats), f32),
                pltpu.VMEM((tiles, lats), f32),
                pltpu.VMEM((2, freqs, lats), f32),
                pltpu.VMEM((freqs, lats), f32),
                pltpu.VMEM((STEPS - 1, 2, 1, lats), f32),
                pltpu.VMEM((STEPS - 1, 2, 1, lats), f32),
                pltpu.VMEM((tiles, lats), f32),
                pltpu.VMEM((tiles, lats), f32),
                pltpu.VMEM((lats, lats), f32),
                pltpu.VMEM((lats, 2 * lats), f32),
                pltpu.VMEM((devices, 1, lats), f32),
                dma((quarter,)),
                dma((3,)),
                dma((STEPS, 2, quarter)),
                dma((STEPS, 2, quarter)),
                dma((STEPS - 1, 2)),
                dma((STEPS - 1, 2)),
                dma,
                dma,
                pltpu.SemaphoreType.REGULAR((5,)),
            ],
            compiler_params=pltpu.CompilerParams(
                collective_id=0, has_side_effects=True, vmem_limit_bytes=KERNEL_VMEM
            ),
        )(
            *(
                pltpu.with_memory_space_constraint(argument, pltpu.HBM)
                for argument in (
                    spectrum.reshape(4, quarter, tiles, lats),
                    wind,
                    land_sea,
                    band_rows.reshape(1, lats),
                )
            )
        )
        next_spectrum, ocean = pl.pallas_call(
            functools.partial(output_kernel, (devices, lons, lats)),
            out_shape=(
                jax.ShapeDtypeStruct((4, quarter, tiles, lats), f32),
                jax.ShapeDtypeStruct((4, 2, devices * lons), f32),
            ),
            in_specs=[vmem_space] * 2,
            out_specs=(hbm_space, hbm_space),
            scratch_shapes=[
                pltpu.VMEM((4, 2, devices * lons), f32),
                dma((4,)),
                dma,
            ],
            compiler_params=pltpu.CompilerParams(vmem_limit_bytes=KERNEL_VMEM),
        )(final, arrived)
        return next_spectrum.reshape(spectrum.shape), ocean

    return jax.shard_map(
        per_device,
        mesh=mesh,
        in_specs=(P(None, None, MEMBER_GX, None), P(None, MEMBER_GX, None), P("gx", None), P(None)),
        out_specs=(P(None, None, MEMBER_GX, None), P(None, "gx", "member")),
        check_vma=False,
    )
```

```python
import functools
import math

import jax
import jax.numpy as jnp
from jax import lax
from jax.experimental import pallas as pl
from jax.experimental.pallas import tpu as pltpu
from jax.sharding import PartitionSpec as P

STEPS = 3
EARLY = (5, 4)
KERNEL_VMEM = 36 * 2**20
HEARD = ((0, 3), (0, 9), (0, 6), (1, 2))
MEMBER_GX = ("member", "gx")
MESH = pl.DeviceIdType.MESH


def freq_constants(freqs):
    out = []
    for j in range(freqs):
        shrink = 1.1 ** (-j)
        weight = (j + 1) / freqs
        inverse_speed = 2.0 * math.pi * (0.0418 / shrink) / 9.81
        out.append((0.45 * shrink, 0.05 * inverse_speed, weight, 0.3 * weight * weight))
    return out


def window_kernel(
    sizes,
    spectrum,
    wind,
    land,
    band,
    buf,
    arrived,
    grow,
    grow_one,
    wind_v,
    land_v,
    band_v,
    trig,
    send_e,
    send_w,
    recv_e,
    recv_w,
    halo,
    damp,
    damp_edge,
    shrink_rows,
    edge_send,
    edge_recv,
    stokes_c,
    stokes_s,
    place,
    turned,
    message,
    load_sem,
    small_sem,
    halo_send_sem,
    halo_recv_sem,
    edge_send_sem,
    edge_recv_sem,
    message_send_sem,
    message_recv_sem,
    known_sem,
):
    devices, quarter, freqs, lons, lats = sizes
    consts = freq_constants(freqs)
    me = lax.axis_index("gx")
    east = lax.rem(me + 1, devices)
    west = lax.rem(me + devices - 1, devices)

    barrier = pltpu.get_barrier_semaphore()
    for neighbour in (west, east):
        pl.semaphore_signal(barrier, inc=1, device_id={"gx": neighbour}, device_id_type=MESH)

    def load(k):
        return pltpu.make_async_copy(spectrum.at[:, k], buf.at[:, k], load_sem.at[k])

    small = [
        pltpu.make_async_copy(wind, wind_v, small_sem.at[0]),
        pltpu.make_async_copy(land, land_v, small_sem.at[1]),
        pltpu.make_async_copy(band, band_v, small_sem.at[2]),
    ]
    for copy in small:
        copy.start()

    for k in range(quarter):
        load(k).start()

    for k in range(quarter):
        angle = (k + 0.5) * 2.0 * math.pi / (4 * quarter)
        trig[k] = jnp.float32(math.cos(angle))
        trig[quarter + k] = jnp.float32(math.sin(angle))
    rows = lax.broadcasted_iota(jnp.int32, (lons, lats), 0)
    lanes = lax.broadcasted_iota(jnp.int32, (lons, lats), 1)
    first_row = jnp.where(rows == 0, 1.0, 0.0)
    last_row = jnp.where(rows == lons - 1, 1.0, 0.0)
    inner_south = jnp.where(lanes == 0, 0.0, 1.0)
    inner_north = jnp.where(lanes == lats - 1, 0.0, 1.0)
    stokes_c[...] = jnp.zeros_like(stokes_c)
    stokes_s[...] = jnp.zeros_like(stokes_s)
    turned[...] = jnp.zeros_like(turned)
    for j in range(freqs):
        line = jnp.full((1, lats), consts[j][0], jnp.float32)
        for rows_of in (shrink_rows, damp_edge.at[0], damp_edge.at[1]):
            rows_of[pl.ds(j, 1)] = line

    with jax.named_scope("barrier_wait"):
        pl.semaphore_wait(barrier, 2)

    def tell(n):
        reach = 2**n
        for other in (lax.rem(me + reach, devices), lax.rem(me + devices - reach, devices)):
            pl.semaphore_signal(known_sem.at[n], inc=1, device_id={"gx": other}, device_id_type=MESH)

    def hear(n):
        pl.semaphore_wait(known_sem.at[n], 2)

    rounds = 5
    assert 2 ** (rounds + 1) == devices
    tell(0)

    def halo_copy(s, k, to_east):
        src, dst, side, where = (send_e, recv_e, 0, east) if to_east else (send_w, recv_w, 1, west)
        return pltpu.make_async_remote_copy(
            src_ref=src.at[s, k],
            dst_ref=dst.at[s, k],
            send_sem=halo_send_sem.at[s, side, k],
            recv_sem=halo_recv_sem.at[s, side, k],
            device_id={"gx": where},
            device_id_type=MESH,
        )

    def edge_copy(s, to_east):
        side, where = (0, east) if to_east else (1, west)
        return pltpu.make_async_remote_copy(
            src_ref=edge_send.at[s, side],
            dst_ref=edge_recv.at[s, side],
            send_sem=edge_send_sem.at[s, side],
            recv_sem=edge_recv_sem.at[s, side],
            device_id={"gx": where},
            device_id_type=MESH,
        )

    def pack(s, k):
        last = pl.ds(lons - 1, freqs, stride=lons)
        first = pl.ds(0, freqs, stride=lons)
        send_e[s, k, :freqs] = buf[0, k, last]
        send_e[s, k, freqs:] = buf[3, k, last]
        send_w[s, k, :freqs] = buf[1, k, first]
        send_w[s, k, freqs:] = buf[2, k, first]

    def ship(s, k):
        halo_copy(s, k, True).start()
        halo_copy(s, k, False).start()

    with jax.named_scope("first_ship"):
        @pl.loop(0, quarter)
        def _(k):
            load(k).wait()
            pack(0, k)
            ship(0, k)

    for copy in small:
        copy.wait()
    mask = land_v[...].astype(jnp.float32)
    wind_east = wind_v[0]
    wind_north = wind_v[1]

    def body(s, mode, k, carry):
        energy, across, along = carry
        c = jnp.full((lons, lats), trig[k], jnp.float32)
        n = jnp.full((lons, lats), trig[quarter + k], jnp.float32)
        both = c + n
        y_rates = ((n * inner_south, c * inner_south), (n * inner_north, c * inner_north))
        x_rates = (c, n, c, n)
        sides = (0, 1, 1, 0)
        if mode == "finish":
            halo_copy(s, k, True).wait_recv()
            halo_copy(s, k, False).wait_recv()
            for heard in (2, 3):
                if HEARD[heard][0] == s:

                    @pl.when(k == HEARD[heard][1])
                    def _(heard=heard):
                        hear(heard)
                        tell(heard + 1)

            for side, got in ((0, recv_e), (1, recv_w)):
                scale = damp_edge[side]
                halo[side, :freqs] = got[s, k, :freqs] * scale
                halo[side, freqs:] = got[s, k, freqs:] * scale
            outer = [x_rates[q] * (first_row, last_row)[sides[q]] for q in range(4)]
        else:
            inner = [x_rates[q] * (1.0 - (first_row, last_row)[sides[q]]) for q in range(4)]
            if s == 0:

                @pl.when(k == HEARD[0][1])
                def _():
                    hear(0)
                    tell(1)

                blow = wind_east * c + wind_north * n
                cross = wind_north * c - wind_east * n
        sum_across = jnp.zeros((lons, lats), jnp.float32)
        sum_along = jnp.zeros((lons, lats), jnp.float32)
        energy = list(energy)
        for j in range(freqs):
            shrink, speed, weight, _ = consts[j]
            tile = pl.ds(j * lons, lons)
            if mode != "finish":
                if s > 0:
                    d = damp[tile]
                else:
                    ahead = blow * speed
                    aside = cross * speed
                    gains = (ahead - 0.05, aside - 0.05, -0.05 - ahead, -0.05 - aside)
            new, flux = [], []
            for q in range(4):
                if mode == "finish":
                    moved = buf[q, k, tile]
                else:
                    center = buf[q, k, tile]
                    if s > 0:
                        center = center * d
                    upwind_x = pltpu.roll(center, lons - 1 if sides[q] else 1, 0)
                    upwind_y = pltpu.roll(center, 1 if q < 2 else lats - 1, 1)
                    change = both * center - inner[q] * upwind_x - y_rates[q // 2][q % 2] * upwind_y
                    moved = center - shrink * change
                    if s == 0:
                        gain = mask * jnp.minimum(jnp.maximum(gains[q], 0.0), 0.2)
                        grow[q, k, tile] = gain
                        gain_one = gain + mask
                        grow_one[q, k, tile] = gain_one
                if mode == "start":
                    buf[q, k, tile] = moved
                    continue
                row = j + (freqs if q >= 2 else 0)
                moved = moved + outer[q] * halo[sides[q], pl.ds(row, 1)]
                energy[q] = energy[q] + moved
                value = moved * grow_one[q, k, tile]
                buf[q, k, tile] = value
                if s == STEPS - 1:
                    new.append(value)
                    flux.append(moved * grow[q, k, tile])
            if s == STEPS - 1 and mode == "finish":
                sum_across = sum_across + weight * (flux[0] - flux[2])
                sum_along = sum_along + weight * (flux[1] - flux[3])
                d02 = new[0] - new[2]
                d13 = new[1] - new[3]
                stokes_c[tile] = stokes_c[tile] + (c * d02 - n * d13)
                stokes_s[tile] = stokes_s[tile] + (n * d02 + c * d13)
        if mode == "start":
            return carry
        across = across + (c * sum_across - n * sum_along)
        along = along + (n * sum_across + c * sum_along)
        if s < STEPS - 1:
            pack(s + 1, k)

            @pl.when(k < EARLY[s])
            def _():
                ship(s + 1, k)

        return tuple(energy), across, along

    zero = jnp.zeros((lons, lats), jnp.float32)
    nothing = ((zero,) * 4, zero, zero)

    def start_step(s):
        lax.fori_loop(0, quarter, functools.partial(body, s, "start"), nothing)

    def finish_step(s):
        energy, across, along = lax.fori_loop(
            0, quarter, functools.partial(body, s, "finish"), nothing
        )
        total = (energy[0] + energy[1]) + (energy[2] + energy[3])
        return mask * total * (1.0 / (4 * quarter * freqs)), across, along

    def set_damping(energy):
        ratio = energy / (0.5 + energy)
        for j in range(freqs):
            damp[pl.ds(j * lons, lons)] = 1.0 / (1.0 + consts[j][3] * ratio)

    with jax.named_scope("start0"):
        start_step(0)
    hear(1)
    tell(2)
    edge_weight = (lax.broadcasted_iota(jnp.int32, (freqs, lats), 0).astype(jnp.float32) + 1.0) / freqs
    edge_weight = 0.3 * edge_weight * edge_weight

    for s in range(STEPS):
        with jax.named_scope(f"step{s}"):
            energy, across, along = finish_step(s)
        if s < STEPS - 1:
            edge_send[s, 0] = energy[lons - 1 :]
            edge_send[s, 1] = energy[:1]
            edge_copy(s, True).start()
            edge_copy(s, False).start()
            for k in range(EARLY[s], quarter):
                ship(s + 1, k)
        set_damping(energy)
        if s == 0:
            lat = lax.broadcasted_iota(jnp.int32, (lats, lats), 0)
            place[...] = jnp.where(band_v[...] == lat, 1.0, 0.0).T
        if s < STEPS - 1:
            with jax.named_scope(f"start{s + 1}"):
                start_step(s + 1)
            for side, to_east in ((0, True), (1, False)):
                with jax.named_scope(f"edge{s}{side}"):
                    edge_copy(s, to_east).wait_recv()
                other = edge_recv[s, side]
                ratio = other / (0.5 + other)
                damp_edge[side] = shrink_rows[...] / (1.0 + edge_weight * ratio)

    with jax.named_scope("fields"):
        factor = 3.0 / math.sqrt(4 * quarter * freqs)
        drift_c = jnp.zeros((lons, lats), jnp.float32)
        drift_s = jnp.zeros((lons, lats), jnp.float32)
        for j in range(freqs):
            tile = pl.ds(j * lons, lons)
            d = damp[tile] * consts[j][2]
            drift_c = drift_c + d * stokes_c[tile]
            drift_s = drift_s + d * stokes_s[tile]
        parts = 4 * lons
        for c, value in enumerate((across, along, drift_c, drift_s)):
            value = factor * value
            turned[pl.ds(c * lons, lons), :lats] = value
            turned[pl.ds(parts + c * lons, lons), lats:] = value
        pick = jnp.concatenate(
            [place[pl.ds(0, devices, stride=2)], place[pl.ds(1, devices, stride=2)]], axis=1
        )
        message[:, 0, :] = lax.dot_general(
            pick,
            turned[...],
            (((1,), (1,)), ((), ())),
            precision=lax.Precision.HIGHEST,
            preferred_element_type=jnp.float32,
        )[:, : 2 * parts]

    with jax.named_scope("hear"):
        hear(rounds - 1)

    def message_copy(offset):
        to = lax.rem(me + offset, devices)
        return pltpu.make_async_remote_copy(
            src_ref=message.at[to],
            dst_ref=arrived.at[me],
            send_sem=message_send_sem,
            recv_sem=message_recv_sem,
            device_id={"gx": to},
            device_id_type=MESH,
        )

    with jax.named_scope("issue"):
        half = devices // 2
        message_copy(half).start()

        @pl.loop(1, half)
        def _(near):
            message_copy(half - near).start()
            message_copy(half + near).start()

    arrived[me] = message[me]

    @pl.loop(0, quarter)
    def _(k):
        for j in range(freqs):
            tile = pl.ds(j * lons, lons)
            d = damp[tile]
            for q in range(4):
                buf[q, k, tile] = buf[q, k, tile] * d

    for s in range(STEPS):
        for k in range(quarter):
            halo_copy(s, k, True).wait_send()
            halo_copy(s, k, False).wait_send()
    for s in range(STEPS - 1):
        edge_copy(s, True).wait_send()
        edge_copy(s, False).wait_send()
    all_out = pltpu.make_async_remote_copy(
        src_ref=message.at[pl.ds(0, devices - 1)],
        dst_ref=arrived.at[pl.ds(0, devices - 1)],
        send_sem=message_send_sem,
        recv_sem=message_recv_sem,
        device_id={"gx": east},
        device_id_type=MESH,
    )
    with jax.named_scope("wait_send"):
        all_out.wait_send()
    with jax.named_scope("wait_recv"):
        all_out.wait_recv()


def output_kernel(sizes, spectrum, arrived, spectrum_out, ocean_out, ocean, store_sem, ocean_sem):
    devices, lons, lats = sizes
    stores = [
        pltpu.make_async_copy(spectrum.at[q], spectrum_out.at[q], store_sem.at[q]) for q in range(4)
    ]
    for copy in stores:
        copy.start()
    rows = lax.broadcasted_iota(jnp.int32, (8, lats), 0)
    block = lax.broadcasted_iota(jnp.int32, (8, lats), 1) // lons
    per = lats // lons
    ahead = lax.rem(block - rows + per, per)
    wanted = [ahead == n for n in range(per)]
    for b in range(devices // per):
        pieces = []
        for h in range(per // 8):
            piece = arrived[pl.ds(b * per + h * 8, 8), 0, :]
            piece = jnp.concatenate([piece, jnp.zeros_like(piece)], axis=1)
            pieces.append(pltpu.roll(piece, h * 8 * lons, 1, stride=lons, stride_axis=0))
        for slot in range(8):
            total = jnp.zeros((8, lats), jnp.float32)
            for h, piece in enumerate(pieces):
                total = total + jnp.where(wanted[(slot + h * 8) % per], piece, 0.0)
            line = jnp.sum(total, axis=0, keepdims=True)
            if slot:
                line = pltpu.roll(jnp.broadcast_to(line, (8, lats)), lats - slot * lons, 1)[:1]
            r, c = divmod(slot, 4)
            ocean[c, pl.ds(r, 1), pl.ds(b * lats, lats)] = line
    last = pltpu.make_async_copy(ocean, ocean_out, ocean_sem)
    last.start()
    last.wait()
    for copy in stores:
        copy.wait()


def solution(mesh):
    devices = mesh.shape["gx"]

    def per_device(spectrum, wind, land_sea, band_rows):
        dirs, freqs, lons, lats = spectrum.shape
        quarter = dirs // 4
        tiles = freqs * lons
        f32 = jnp.float32
        hbm_space = pl.BlockSpec(memory_space=pltpu.HBM)
        vmem_space = pl.BlockSpec(memory_space=pltpu.VMEM)
        dma = pltpu.SemaphoreType.DMA
        final, arrived = pl.pallas_call(
            functools.partial(window_kernel, (devices, quarter, freqs, lons, lats)),
            out_shape=(
                pltpu.VMEM((4, quarter, tiles, lats), f32),
                pltpu.VMEM((devices, 1, 8 * lons), f32),
            ),
            in_specs=[hbm_space] * 4,
            out_specs=(vmem_space, vmem_space),
            scratch_shapes=[
                pltpu.VMEM((4, quarter, tiles, lats), f32),
                pltpu.VMEM((4, quarter, tiles, lats), f32),
                pltpu.VMEM((2, lons, lats), f32),
                pltpu.VMEM((lons, lats), jnp.int32),
                pltpu.VMEM((1, lats), jnp.int32),
                pltpu.SMEM((2 * quarter,), f32),
                pltpu.VMEM((STEPS, quarter, 2 * freqs, lats), f32),
                pltpu.VMEM((STEPS, quarter, 2 * freqs, lats), f32),
                pltpu.VMEM((STEPS, quarter, 2 * freqs, lats), f32),
                pltpu.VMEM((STEPS, quarter, 2 * freqs, lats), f32),
                pltpu.VMEM((2, 2 * freqs, lats), f32),
                pltpu.VMEM((tiles, lats), f32),
                pltpu.VMEM((2, freqs, lats), f32),
                pltpu.VMEM((freqs, lats), f32),
                pltpu.VMEM((STEPS - 1, 2, 1, lats), f32),
                pltpu.VMEM((STEPS - 1, 2, 1, lats), f32),
                pltpu.VMEM((tiles, lats), f32),
                pltpu.VMEM((tiles, lats), f32),
                pltpu.VMEM((lats, lats), f32),
                pltpu.VMEM((lats, 2 * lats), f32),
                pltpu.VMEM((devices, 1, 8 * lons), f32),
                dma((quarter,)),
                dma((3,)),
                dma((STEPS, 2, quarter)),
                dma((STEPS, 2, quarter)),
                dma((STEPS - 1, 2)),
                dma((STEPS - 1, 2)),
                dma,
                dma,
                pltpu.SemaphoreType.REGULAR((5,)),
            ],
            compiler_params=pltpu.CompilerParams(
                collective_id=0, has_side_effects=True, vmem_limit_bytes=KERNEL_VMEM
            ),
        )(
            *(
                pltpu.with_memory_space_constraint(argument, pltpu.HBM)
                for argument in (
                    spectrum.reshape(4, quarter, tiles, lats),
                    wind,
                    land_sea,
                    band_rows.reshape(1, lats),
                )
            )
        )
        next_spectrum, ocean = pl.pallas_call(
            functools.partial(output_kernel, (devices, lons, lats)),
            out_shape=(
                jax.ShapeDtypeStruct((4, quarter, tiles, lats), f32),
                jax.ShapeDtypeStruct((4, 2, devices * lons), f32),
            ),
            in_specs=[vmem_space] * 2,
            out_specs=(hbm_space, hbm_space),
            scratch_shapes=[
                pltpu.VMEM((4, 2, devices * lons), f32),
                dma((4,)),
                dma,
            ],
            compiler_params=pltpu.CompilerParams(vmem_limit_bytes=KERNEL_VMEM),
        )(final, arrived)
        return next_spectrum.reshape(spectrum.shape), ocean

    return jax.shard_map(
        per_device,
        mesh=mesh,
        in_specs=(P(None, None, MEMBER_GX, None), P(None, MEMBER_GX, None), P("gx", None), P(None)),
        out_specs=(P(None, None, MEMBER_GX, None), P(None, "gx", "member")),
        check_vma=False,
    )
```

```python
import functools
import math

import jax
import jax.numpy as jnp
from jax import lax
from jax.experimental import pallas as pl
from jax.experimental.pallas import tpu as pltpu
from jax.sharding import PartitionSpec as P

STEPS = 3
EARLY = (5, 4)
KERNEL_VMEM = 36 * 2**20
HEARD = ((0, 3), (0, 9), (0, 6), (1, 2))
MEMBER_GX = ("member", "gx")
MESH = pl.DeviceIdType.MESH


def freq_constants(freqs):
    out = []
    for j in range(freqs):
        shrink = 1.1 ** (-j)
        weight = (j + 1) / freqs
        inverse_speed = 2.0 * math.pi * (0.0418 / shrink) / 9.81
        out.append((0.45 * shrink, 0.05 * inverse_speed, weight, 0.3 * weight * weight))
    return out


def window_kernel(
    sizes,
    spectrum,
    columns,
    wind,
    land,
    band,
    buf,
    arrived,
    grow,
    grow_one,
    wind_v,
    land_v,
    band_v,
    trig,
    send_e,
    send_w,
    recv_e,
    recv_w,
    halo,
    damp,
    damp_edge,
    shrink_rows,
    edge_send,
    edge_recv,
    stokes_c,
    stokes_s,
    place,
    turned,
    message,
    load_sem,
    bound_sem,
    small_sem,
    halo_send_sem,
    halo_recv_sem,
    edge_send_sem,
    edge_recv_sem,
    message_send_sem,
    message_recv_sem,
    known_sem,
):
    devices, quarter, freqs, lons, lats = sizes
    consts = freq_constants(freqs)
    me = lax.axis_index("gx")
    east = lax.rem(me + 1, devices)
    west = lax.rem(me + devices - 1, devices)

    barrier = pltpu.get_barrier_semaphore()
    for neighbour in (west, east):
        pl.semaphore_signal(barrier, inc=1, device_id={"gx": neighbour}, device_id_type=MESH)

    def load(k):
        return pltpu.make_async_copy(spectrum.at[:, k], buf.at[:, k], load_sem.at[k])

    small = [
        pltpu.make_async_copy(wind, wind_v, small_sem.at[0]),
        pltpu.make_async_copy(land, land_v, small_sem.at[1]),
        pltpu.make_async_copy(band, band_v, small_sem.at[2]),
    ]
    for copy in small:
        copy.start()

    bounds = [
        pltpu.make_async_copy(
            columns.at[q, :, :, lon], to.at[0, :, pl.ds(half * freqs, freqs)], bound_sem.at[q]
        )
        for q, to, half, lon in (
            (0, send_e, 0, lons - 1),
            (1, send_w, 0, 0),
            (2, send_w, 1, 0),
            (3, send_e, 1, lons - 1),
        )
    ]
    for copy in bounds:
        copy.start()
    for k in range(quarter):
        load(k).start()

    for k in range(quarter):
        angle = (k + 0.5) * 2.0 * math.pi / (4 * quarter)
        trig[k] = jnp.float32(math.cos(angle))
        trig[quarter + k] = jnp.float32(math.sin(angle))
    rows = lax.broadcasted_iota(jnp.int32, (lons, lats), 0)
    lanes = lax.broadcasted_iota(jnp.int32, (lons, lats), 1)
    first_row = jnp.where(rows == 0, 1.0, 0.0)
    last_row = jnp.where(rows == lons - 1, 1.0, 0.0)
    inner_south = jnp.where(lanes == 0, 0.0, 1.0)
    inner_north = jnp.where(lanes == lats - 1, 0.0, 1.0)
    stokes_c[...] = jnp.zeros_like(stokes_c)
    stokes_s[...] = jnp.zeros_like(stokes_s)
    turned[...] = jnp.zeros_like(turned)
    for j in range(freqs):
        line = jnp.full((1, lats), consts[j][0], jnp.float32)
        for rows_of in (shrink_rows, damp_edge.at[0], damp_edge.at[1]):
            rows_of[pl.ds(j, 1)] = line

    with jax.named_scope("barrier_wait"):
        pl.semaphore_wait(barrier, 2)

    def tell(n):
        reach = 2**n
        for other in (lax.rem(me + reach, devices), lax.rem(me + devices - reach, devices)):
            pl.semaphore_signal(known_sem.at[n], inc=1, device_id={"gx": other}, device_id_type=MESH)

    def hear(n):
        pl.semaphore_wait(known_sem.at[n], 2)

    rounds = 5
    assert 2 ** (rounds + 1) == devices
    tell(0)

    def halo_copy(s, k, to_east):
        src, dst, side, where = (send_e, recv_e, 0, east) if to_east else (send_w, recv_w, 1, west)
        return pltpu.make_async_remote_copy(
            src_ref=src.at[s, k],
            dst_ref=dst.at[s, k],
            send_sem=halo_send_sem.at[s, side, k],
            recv_sem=halo_recv_sem.at[s, side, k],
            device_id={"gx": where},
            device_id_type=MESH,
        )

    def edge_copy(s, to_east):
        side, where = (0, east) if to_east else (1, west)
        return pltpu.make_async_remote_copy(
            src_ref=edge_send.at[s, side],
            dst_ref=edge_recv.at[s, side],
            send_sem=edge_send_sem.at[s, side],
            recv_sem=edge_recv_sem.at[s, side],
            device_id={"gx": where},
            device_id_type=MESH,
        )

    def pack(s, k):
        last = pl.ds(lons - 1, freqs, stride=lons)
        first = pl.ds(0, freqs, stride=lons)
        send_e[s, k, :freqs] = buf[0, k, last]
        send_e[s, k, freqs:] = buf[3, k, last]
        send_w[s, k, :freqs] = buf[1, k, first]
        send_w[s, k, freqs:] = buf[2, k, first]

    def ship(s, k):
        halo_copy(s, k, True).start()
        halo_copy(s, k, False).start()

    with jax.named_scope("first_ship"):
        for copy in bounds:
            copy.wait()

        @pl.loop(0, quarter)
        def _(k):
            ship(0, k)

    for copy in small:
        copy.wait()
    mask = land_v[...].astype(jnp.float32)
    wind_east = wind_v[0]
    wind_north = wind_v[1]

    def body(s, mode, k, carry):
        energy, across, along = carry
        c = jnp.full((lons, lats), trig[k], jnp.float32)
        n = jnp.full((lons, lats), trig[quarter + k], jnp.float32)
        both = c + n
        y_rates = ((n * inner_south, c * inner_south), (n * inner_north, c * inner_north))
        x_rates = (c, n, c, n)
        sides = (0, 1, 1, 0)
        if mode == "finish":
            halo_copy(s, k, True).wait_recv()
            halo_copy(s, k, False).wait_recv()
            for heard in (2, 3):
                if HEARD[heard][0] == s:

                    @pl.when(k == HEARD[heard][1])
                    def _(heard=heard):
                        hear(heard)
                        tell(heard + 1)

            for side, got in ((0, recv_e), (1, recv_w)):
                scale = damp_edge[side]
                halo[side, :freqs] = got[s, k, :freqs] * scale
                halo[side, freqs:] = got[s, k, freqs:] * scale
            outer = [x_rates[q] * (first_row, last_row)[sides[q]] for q in range(4)]
        else:
            inner = [x_rates[q] * (1.0 - (first_row, last_row)[sides[q]]) for q in range(4)]
            if s == 0:
                load(k).wait()

                @pl.when(k == HEARD[0][1])
                def _():
                    hear(0)
                    tell(1)

                blow = wind_east * c + wind_north * n
                cross = wind_north * c - wind_east * n
        sum_across = jnp.zeros((lons, lats), jnp.float32)
        sum_along = jnp.zeros((lons, lats), jnp.float32)
        energy = list(energy)
        for j in range(freqs):
            shrink, speed, weight, _ = consts[j]
            tile = pl.ds(j * lons, lons)
            if mode != "finish":
                if s > 0:
                    d = damp[tile]
                else:
                    ahead = blow * speed
                    aside = cross * speed
                    gains = (ahead - 0.05, aside - 0.05, -0.05 - ahead, -0.05 - aside)
            new, flux = [], []
            for q in range(4):
                if mode == "finish":
                    moved = buf[q, k, tile]
                else:
                    center = buf[q, k, tile]
                    if s > 0:
                        center = center * d
                    upwind_x = pltpu.roll(center, lons - 1 if sides[q] else 1, 0)
                    upwind_y = pltpu.roll(center, 1 if q < 2 else lats - 1, 1)
                    change = both * center - inner[q] * upwind_x - y_rates[q // 2][q % 2] * upwind_y
                    moved = center - shrink * change
                    if s == 0:
                        gain = mask * jnp.minimum(jnp.maximum(gains[q], 0.0), 0.2)
                        grow[q, k, tile] = gain
                        gain_one = gain + mask
                        grow_one[q, k, tile] = gain_one
                if mode == "start":
                    buf[q, k, tile] = moved
                    continue
                row = j + (freqs if q >= 2 else 0)
                moved = moved + outer[q] * halo[sides[q], pl.ds(row, 1)]
                energy[q] = energy[q] + moved
                value = moved * grow_one[q, k, tile]
                buf[q, k, tile] = value
                if s == STEPS - 1:
                    new.append(value)
                    flux.append(moved * grow[q, k, tile])
            if s == STEPS - 1 and mode == "finish":
                sum_across = sum_across + weight * (flux[0] - flux[2])
                sum_along = sum_along + weight * (flux[1] - flux[3])
                d02 = new[0] - new[2]
                d13 = new[1] - new[3]
                stokes_c[tile] = stokes_c[tile] + (c * d02 - n * d13)
                stokes_s[tile] = stokes_s[tile] + (n * d02 + c * d13)
        if mode == "start":
            return carry
        across = across + (c * sum_across - n * sum_along)
        along = along + (n * sum_across + c * sum_along)
        if s < STEPS - 1:
            pack(s + 1, k)

            @pl.when(k < EARLY[s])
            def _():
                ship(s + 1, k)

        return tuple(energy), across, along

    zero = jnp.zeros((lons, lats), jnp.float32)
    nothing = ((zero,) * 4, zero, zero)

    def start_step(s):
        lax.fori_loop(0, quarter, functools.partial(body, s, "start"), nothing)

    def finish_step(s):
        energy, across, along = lax.fori_loop(
            0, quarter, functools.partial(body, s, "finish"), nothing
        )
        total = (energy[0] + energy[1]) + (energy[2] + energy[3])
        return mask * total * (1.0 / (4 * quarter * freqs)), across, along

    def set_damping(energy):
        ratio = energy / (0.5 + energy)
        for j in range(freqs):
            damp[pl.ds(j * lons, lons)] = 1.0 / (1.0 + consts[j][3] * ratio)

    with jax.named_scope("start0"):
        start_step(0)
    hear(1)
    tell(2)
    edge_weight = (lax.broadcasted_iota(jnp.int32, (freqs, lats), 0).astype(jnp.float32) + 1.0) / freqs
    edge_weight = 0.3 * edge_weight * edge_weight

    for s in range(STEPS):
        with jax.named_scope(f"step{s}"):
            energy, across, along = finish_step(s)
        if s < STEPS - 1:
            edge_send[s, 0] = energy[lons - 1 :]
            edge_send[s, 1] = energy[:1]
            edge_copy(s, True).start()
            edge_copy(s, False).start()
            for k in range(EARLY[s], quarter):
                ship(s + 1, k)
        set_damping(energy)
        if s == 0:
            lat = lax.broadcasted_iota(jnp.int32, (lats, lats), 0)
            place[...] = jnp.where(band_v[...] == lat, 1.0, 0.0).T
        if s < STEPS - 1:
            with jax.named_scope(f"start{s + 1}"):
                start_step(s + 1)
            for side, to_east in ((0, True), (1, False)):
                with jax.named_scope(f"edge{s}{side}"):
                    edge_copy(s, to_east).wait_recv()
                other = edge_recv[s, side]
                ratio = other / (0.5 + other)
                damp_edge[side] = shrink_rows[...] / (1.0 + edge_weight * ratio)

    with jax.named_scope("fields"):
        factor = 3.0 / math.sqrt(4 * quarter * freqs)
        drift_c = jnp.zeros((lons, lats), jnp.float32)
        drift_s = jnp.zeros((lons, lats), jnp.float32)
        for j in range(freqs):
            tile = pl.ds(j * lons, lons)
            d = damp[tile] * consts[j][2]
            drift_c = drift_c + d * stokes_c[tile]
            drift_s = drift_s + d * stokes_s[tile]
        parts = 4 * lons
        for c, value in enumerate((across, along, drift_c, drift_s)):
            value = factor * value
            turned[pl.ds(c * lons, lons), :lats] = value
            turned[pl.ds(parts + c * lons, lons), lats:] = value
        pick = jnp.concatenate(
            [place[pl.ds(0, devices, stride=2)], place[pl.ds(1, devices, stride=2)]], axis=1
        )
        message[:, 0, :] = lax.dot_general(
            pick,
            turned[...],
            (((1,), (1,)), ((), ())),
            precision=lax.Precision.HIGHEST,
            preferred_element_type=jnp.float32,
        )[:, : 2 * parts]

    with jax.named_scope("hear"):
        hear(rounds - 1)

    def message_copy(offset):
        to = lax.rem(me + offset, devices)
        return pltpu.make_async_remote_copy(
            src_ref=message.at[to],
            dst_ref=arrived.at[me],
            send_sem=message_send_sem,
            recv_sem=message_recv_sem,
            device_id={"gx": to},
            device_id_type=MESH,
        )

    with jax.named_scope("issue"):
        half = devices // 2
        message_copy(half).start()

        @pl.loop(1, half)
        def _(near):
            message_copy(half - near).start()
            message_copy(half + near).start()

    arrived[me] = message[me]

    @pl.loop(0, quarter)
    def _(k):
        for j in range(freqs):
            tile = pl.ds(j * lons, lons)
            d = damp[tile]
            for q in range(4):
                buf[q, k, tile] = buf[q, k, tile] * d

    for s in range(STEPS):
        for k in range(quarter):
            halo_copy(s, k, True).wait_send()
            halo_copy(s, k, False).wait_send()
    for s in range(STEPS - 1):
        edge_copy(s, True).wait_send()
        edge_copy(s, False).wait_send()
    all_out = pltpu.make_async_remote_copy(
        src_ref=message.at[pl.ds(0, devices - 1)],
        dst_ref=arrived.at[pl.ds(0, devices - 1)],
        send_sem=message_send_sem,
        recv_sem=message_recv_sem,
        device_id={"gx": east},
        device_id_type=MESH,
    )
    with jax.named_scope("wait_send"):
        all_out.wait_send()
    with jax.named_scope("wait_recv"):
        all_out.wait_recv()


def output_kernel(sizes, spectrum, arrived, spectrum_out, ocean_out, ocean, store_sem, ocean_sem):
    devices, lons, lats = sizes
    stores = [
        pltpu.make_async_copy(spectrum.at[q], spectrum_out.at[q], store_sem.at[q]) for q in range(4)
    ]
    for copy in stores:
        copy.start()
    rows = lax.broadcasted_iota(jnp.int32, (8, lats), 0)
    block = lax.broadcasted_iota(jnp.int32, (8, lats), 1) // lons
    per = lats // lons
    ahead = lax.rem(block - rows + per, per)
    wanted = [ahead == n for n in range(per)]
    for b in range(devices // per):
        pieces = []
        for h in range(per // 8):
            piece = arrived[pl.ds(b * per + h * 8, 8), 0, :]
            piece = jnp.concatenate([piece, jnp.zeros_like(piece)], axis=1)
            pieces.append(pltpu.roll(piece, h * 8 * lons, 1, stride=lons, stride_axis=0))
        for slot in range(8):
            total = jnp.zeros((8, lats), jnp.float32)
            for h, piece in enumerate(pieces):
                total = total + jnp.where(wanted[(slot + h * 8) % per], piece, 0.0)
            line = jnp.sum(total, axis=0, keepdims=True)
            if slot:
                line = pltpu.roll(jnp.broadcast_to(line, (8, lats)), lats - slot * lons, 1)[:1]
            r, c = divmod(slot, 4)
            ocean[c, pl.ds(r, 1), pl.ds(b * lats, lats)] = line
    last = pltpu.make_async_copy(ocean, ocean_out, ocean_sem)
    last.start()
    last.wait()
    for copy in stores:
        copy.wait()


def solution(mesh):
    devices = mesh.shape["gx"]

    def per_device(spectrum, wind, land_sea, band_rows):
        dirs, freqs, lons, lats = spectrum.shape
        quarter = dirs // 4
        tiles = freqs * lons
        f32 = jnp.float32
        hbm_space = pl.BlockSpec(memory_space=pltpu.HBM)
        vmem_space = pl.BlockSpec(memory_space=pltpu.VMEM)
        dma = pltpu.SemaphoreType.DMA
        final, arrived = pl.pallas_call(
            functools.partial(window_kernel, (devices, quarter, freqs, lons, lats)),
            out_shape=(
                pltpu.VMEM((4, quarter, tiles, lats), f32),
                pltpu.VMEM((devices, 1, 8 * lons), f32),
            ),
            in_specs=[hbm_space] * 5,
            out_specs=(vmem_space, vmem_space),
            scratch_shapes=[
                pltpu.VMEM((4, quarter, tiles, lats), f32),
                pltpu.VMEM((4, quarter, tiles, lats), f32),
                pltpu.VMEM((2, lons, lats), f32),
                pltpu.VMEM((lons, lats), jnp.int32),
                pltpu.VMEM((1, lats), jnp.int32),
                pltpu.SMEM((2 * quarter,), f32),
                pltpu.VMEM((STEPS, quarter, 2 * freqs, lats), f32),
                pltpu.VMEM((STEPS, quarter, 2 * freqs, lats), f32),
                pltpu.VMEM((STEPS, quarter, 2 * freqs, lats), f32),
                pltpu.VMEM((STEPS, quarter, 2 * freqs, lats), f32),
                pltpu.VMEM((2, 2 * freqs, lats), f32),
                pltpu.VMEM((tiles, lats), f32),
                pltpu.VMEM((2, freqs, lats), f32),
                pltpu.VMEM((freqs, lats), f32),
                pltpu.VMEM((STEPS - 1, 2, 1, lats), f32),
                pltpu.VMEM((STEPS - 1, 2, 1, lats), f32),
                pltpu.VMEM((tiles, lats), f32),
                pltpu.VMEM((tiles, lats), f32),
                pltpu.VMEM((lats, lats), f32),
                pltpu.VMEM((lats, 2 * lats), f32),
                pltpu.VMEM((devices, 1, 8 * lons), f32),
                dma((quarter,)),
                dma((4,)),
                dma((3,)),
                dma((STEPS, 2, quarter)),
                dma((STEPS, 2, quarter)),
                dma((STEPS - 1, 2)),
                dma((STEPS - 1, 2)),
                dma,
                dma,
                pltpu.SemaphoreType.REGULAR((5,)),
            ],
            compiler_params=pltpu.CompilerParams(
                collective_id=0, has_side_effects=True, vmem_limit_bytes=KERNEL_VMEM
            ),
        )(
            *(
                pltpu.with_memory_space_constraint(argument, pltpu.HBM)
                for argument in (
                    spectrum.reshape(4, quarter, tiles, lats),
                    spectrum.reshape(4, quarter, freqs, lons, lats),
                    wind,
                    land_sea,
                    band_rows.reshape(1, lats),
                )
            )
        )
        next_spectrum, ocean = pl.pallas_call(
            functools.partial(output_kernel, (devices, lons, lats)),
            out_shape=(
                jax.ShapeDtypeStruct((4, quarter, tiles, lats), f32),
                jax.ShapeDtypeStruct((4, 2, devices * lons), f32),
            ),
            in_specs=[vmem_space] * 2,
            out_specs=(hbm_space, hbm_space),
            scratch_shapes=[
                pltpu.VMEM((4, 2, devices * lons), f32),
                dma((4,)),
                dma,
            ],
            compiler_params=pltpu.CompilerParams(vmem_limit_bytes=KERNEL_VMEM),
        )(final, arrived)
        return next_spectrum.reshape(spectrum.shape), ocean

    return jax.shard_map(
        per_device,
        mesh=mesh,
        in_specs=(P(None, None, MEMBER_GX, None), P(None, MEMBER_GX, None), P("gx", None), P(None)),
        out_specs=(P(None, None, MEMBER_GX, None), P(None, "gx", "member")),
        check_vma=False,
    )
```
